32 devices in a mesh: shard: 8 (over z, core), rep: 4 (over y, x).
Axes of the slice: x: 2, y: 2, z: 4, core: 2. Of those that a mesh axis runs over, the one named last changes fastest.
Arguments:
- tokens: bfloat16 [12288, 5120], P(('shard', 'rep')), may hold values from -700 to 700
- norm_gain: float32 [5120], replicated, may hold values from 0.1 to 1.9
- key_bias: float32 [1024], replicated, may hold values from -4 to 4
- key_weight: bfloat16 [8192, 1024], P('shard'), may hold values from -0.078125 to 0.078125
- cotangent: bfloat16 [12288, 1024], P(('shard', 'rep')), may hold values from -40 to 40
- block_slot: int32 [40], replicated, may hold values from 0 to 63, as said below
Outputs:
- projected: bfloat16 [12288, 1024], P(('shard', 'rep'))
- token_grad: bfloat16 [12288, 5120], P(('shard', 'rep'))
- weight_grad: float32 [8192, 1024], P('shard')
- gain_grad: float32 [5120], replicated
- bias_grad: float32 [1024], replicated
The draws below stay inside these ranges and needn't reach their ends.
Inputs may be any that keep to these rules, and one draw needn't show every extreme that they name: Entries are distinct; block b lies on the device of shard with index block_slot[b] // 8, at its local slot block_slot[b] % 8; in every draw some device holds 8 blocks.
All inputs are finite; a program needn't handle non-finite values.
Results may differ from the reference program's by a relative error of at most 0.013.
Values may be sent and summed in bfloat16 or wider, within the bound.
A program may use at most 128 MiB of HBM per device.

```python
import math
import jax
import jax.numpy as jnp
from jax import lax

D = 5120
KVW = 1024
BLK = 128
TOK_DEV = 384
NBLK = 40
CAP = 8
SLOTS = 64
ALL_TOK = 12288
N_SHARD = 8


def draw_tokens(key, part):
    keys = jax.random.split(key, 3)
    row_scale = jnp.exp(jax.random.uniform(keys[0], (ALL_TOK, 1), minval=0.0, maxval=math.log(10.0)))
    col_scale = jnp.exp(jax.random.uniform(keys[1], (1, D), minval=0.0, maxval=math.log(10.0)))
    base = jnp.clip(jax.random.normal(keys[2], (ALL_TOK, D)), -6.0, 6.0)
    return (base * row_scale * col_scale).astype(jnp.bfloat16)


def draw_cotangent(key, part):
    keys = jax.random.split(key, 1)
    position = jnp.arange(ALL_TOK, dtype=jnp.float32)[:, None] / max(ALL_TOK - 1, 1)
    rising = 1.0 + 2.0 * position
    values = jnp.clip(jax.random.normal(keys[0], (ALL_TOK, KVW)), -6.0, 6.0) * rising
    return values.astype(jnp.bfloat16)


def draw_block_slot(key, part):
    keys = jax.random.split(key, 3)
    full_owner = jax.random.randint(keys[0], (), 0, N_SHARD)
    slot_ids = jnp.arange(SLOTS, dtype=jnp.int32)
    order_slots = jax.random.permutation(keys[1], SLOTS).astype(jnp.int32)
    scores = jnp.where(slot_ids // CAP == full_owner, 0, 1 + order_slots)
    chosen = jnp.argsort(scores, stable=True)[:NBLK].astype(jnp.int32)
    block_order = jax.random.permutation(keys[2], NBLK).astype(jnp.int32)
    return chosen[block_order]


def level_of(key, shape, cuts, low, top_value):
    def one(axis_at, shards_of):
        draws = jax.random.uniform(jax.random.fold_in(jax.random.fold_in(key, 6), axis_at), (shards_of,), jnp.float32, low / len(cuts), top_value / len(cuts))
        return jnp.repeat(jnp.exp(draws), shape[axis_at] // shards_of).reshape((-1,) + (1,) * (len(shape) - axis_at - 1))

    factor_of = one(*cuts[0])
    for cut in cuts[1:]:
        factor_of = factor_of * one(*cut)
    return factor_of


def noise(own_key, dims, deviation, bound, pieces=(), held_as=jnp.bfloat16):
    loudness = level_of(own_key, dims, pieces, -0.22, 0.18) if pieces else 1.0
    drawn = jax.random.normal(own_key, dims, jnp.float32) * deviation * loudness
    return jnp.minimum(jnp.maximum(drawn, -bound), bound).astype(held_as)


def setup_inputs(seed: int = 0) -> dict:
    streams_of = jax.random.split(jax.random.key(seed), 7)
    tokens = draw_tokens(jax.random.fold_in(streams_of[6], 71), 0)
    norm_gain = jnp.clip(1.0 + 0.18 * jax.random.normal(streams_of[1], (D,), jnp.float32), 0.1, 1.9)
    key_bias = noise(streams_of[2], (KVW,), 1.0, 4.0, (), jnp.float32)
    key_weight = noise(streams_of[3], (SLOTS * BLK, KVW), D ** -0.5, 0.078125, ((0, 8),))
    cotangent = draw_cotangent(jax.random.fold_in(streams_of[6], 71), 0)
    block_slot = draw_block_slot(jax.random.fold_in(streams_of[6], 71), 0)
    return dict(tokens=tokens, norm_gain=norm_gain, key_bias=key_bias, key_weight=key_weight, cotangent=cotangent, block_slot=block_slot)


EPS = 1e-06

def normalize(tokens, norm_gain):
    values = tokens.astype(jnp.float32)
    inv_rms = lax.rsqrt(lax.optimization_barrier(jnp.mean(values * values, axis=-1, keepdims=True)) + EPS)
    normed = (values * inv_rms * norm_gain).astype(jnp.bfloat16)
    return (values, inv_rms, normed)

def token_backward(values, inv_rms, grad_normed, norm_gain):
    scaled = grad_normed * norm_gain
    inner = lax.optimization_barrier(jnp.mean(scaled * values, axis=-1, keepdims=True))
    return (inv_rms * (scaled - values * inv_rms * inv_rms * inner)).astype(jnp.bfloat16)

def reference(tokens, norm_gain, key_bias, key_weight, cotangent, block_slot):
    whole_weight = key_weight.reshape(SLOTS, BLK, KVW)[block_slot.astype(jnp.int32)].reshape(D, KVW)
    grad_scale = float(ALL_TOK) ** (-0.5)
    device_count = ALL_TOK // TOK_DEV

    def per_device(totals, blocks):
        tok_rows, cot_rows = blocks
        values, inv_rms, normed = normalize(tok_rows, norm_gain)
        forward = jnp.dot(normed, whole_weight, preferred_element_type=jnp.float32)
        projected = (forward + key_bias).astype(jnp.bfloat16)
        grad_normed = lax.dot_general(cot_rows, whole_weight, (((1,), (1,)), ((), ())), preferred_element_type=jnp.float32)
        token_grad = token_backward(values, inv_rms, grad_normed, norm_gain)
        partial_grad = lax.dot_general(normed, cot_rows, (((0,), (0,)), ((), ())), preferred_element_type=jnp.float32) * grad_scale
        rounded = lax.optimization_barrier(partial_grad.astype(jnp.bfloat16)).astype(jnp.float32)
        gain_term = lax.optimization_barrier(jnp.sum(grad_normed * values * inv_rms, axis=0)) * grad_scale
        bias_term = lax.optimization_barrier(jnp.sum(cot_rows.astype(jnp.float32), axis=0)) * grad_scale
        return ((totals[0] + rounded, totals[1] + gain_term, totals[2] + bias_term), (projected, token_grad))
    start = (jnp.zeros((D, KVW), jnp.float32), jnp.zeros((D,), jnp.float32), jnp.zeros((KVW,), jnp.float32))
    totals, outputs = lax.scan(per_device, start, (tokens.reshape(device_count, TOK_DEV, D), cotangent.reshape(device_count, TOK_DEV, KVW)))
    weight_sum, gain_grad, bias_grad = totals
    projected = outputs[0].reshape(ALL_TOK, KVW)
    token_grad = outputs[1].reshape(ALL_TOK, D)
    weight_grad = jnp.zeros((SLOTS, BLK, KVW), jnp.float32).at[block_slot.astype(jnp.int32)].set(weight_sum.reshape(NBLK, BLK, KVW)).reshape(SLOTS * BLK, KVW)
    return (projected, token_grad, weight_grad, gain_grad, bias_grad)
```

```python
import functools
import jax
import jax.numpy as jnp
from jax import lax
from jax.experimental import pallas as pl
from jax.experimental.pallas import tpu as pltpu
from jax.sharding import PartitionSpec as P

BLK = 128
EPS = 1e-06
NJ = 8
NI = 2
SUB = BLK // NJ
QUAD = 4
MESH = pl.DeviceIdType.MESH
F32 = jnp.float32
BF16 = jnp.bfloat16
COMPUTE = 2

OWN, OWNP, SQ, TERM, SUM, HOP1, HOP2, PLACE, ZUP, ZDN, ZEND, PASS = range(12)
FWD, BWD, AGZ, AGSIDE, AGPART, AGEND, G0, GSTEP, GEND = range(12, 21)
COMMON = (SQ, TERM, FWD, BWD)

TUNED = (
    (
        (OWN, 0, 0), (OWN, 1, 0), (OWN, 2, 0), (OWN, 3, 0), (OWNP, 0, 0), (SQ, 0, 0),
        (TERM, 0, 0), (TERM, 1, 0), (AGZ, 1, 0), (AGSIDE, 1, 0), (SUM, 0, 0), (HOP1, 0, 0),
        (SUM, 1, 0), (HOP1, 1, 0), (SUM, 2, 0), (HOP1, 2, 0), (SUM, 3, 0), (HOP1, 3, 0),
        (SUM, 4, 0), (SUM, 5, 0), (HOP1, 4, 0), (HOP1, 5, 0), (SUM, 6, 0), (SUM, 7, 0),
        (HOP1, 7, 0), (AGZ, 1, 1), (SUM, 0, 1), (SUM, 1, 1), (HOP1, 1, 1), (SUM, 2, 1),
        (SUM, 3, 1), (AGSIDE, 1, 1), (SUM, 4, 1), (SUM, 5, 1), (SUM, 6, 1), (HOP1, 3, 1),
        (SUM, 7, 1), (AGPART, 1, 0), (AGZ, 1, 2), (AGSIDE, 1, 2), (HOP2, 1, 0), (HOP1, 0, 1),
        (AGZ, 1, 3), (HOP2, 3, 0), (AGSIDE, 1, 3), (HOP1, 2, 1), (AGZ, 2, 0), (AGSIDE, 2, 0),
        (HOP2, 0, 0), (HOP2, 2, 0), (AGPART, 1, 1), (AGZ, 2, 1), (HOP2, 4, 0), (AGSIDE, 2, 1),
        (HOP1, 5, 1), (AGPART, 1, 2), (HOP2, 0, 1), (AGZ, 2, 2), (AGSIDE, 2, 2), (HOP2, 1, 1),
        (HOP2, 3, 1), (AGPART, 1, 3), (HOP2, 5, 0), (AGZ, 2, 3), (HOP1, 4, 1), (AGSIDE, 2, 3),
        (AGPART, 2, 0), (HOP2, 7, 0), (AGZ, 3, 0), (AGSIDE, 3, 0), (HOP2, 2, 1), (HOP1, 7, 1),
        (PLACE, 0, 0), (ZUP, 0, 3), (ZUP, 0, 2), (ZUP, 0, 1), (AGPART, 2, 1), (PLACE, 1, 0),
        (ZUP, 1, 3), (ZUP, 1, 2), (ZUP, 1, 1), (AGZ, 3, 1), (AGSIDE, 3, 1), (PLACE, 3, 0),
        (ZUP, 3, 3), (ZUP, 3, 2), (ZUP, 3, 1), (AGPART, 2, 2), (AGZ, 3, 2), (AGSIDE, 3, 2),
        (HOP2, 5, 1), (HOP2, 4, 1), (HOP1, 6, 0), (AGPART, 2, 3), (PLACE, 2, 0), (ZUP, 2, 3),
        (ZUP, 2, 2), (ZUP, 2, 1), (AGZ, 3, 3), (AGSIDE, 3, 3), (HOP1, 6, 1), (ZEND, 1, 0),
        (AGPART, 3, 0), (HOP2, 7, 1), (AGPART, 3, 1), (AGPART, 3, 2), (PLACE, 5, 0), (ZUP, 5, 3),
        (ZUP, 5, 2), (ZUP, 5, 1), (PLACE, 4, 0), (ZUP, 4, 3), (ZUP, 4, 2), (ZUP, 4, 1),
        (HOP2, 6, 0), (AGPART, 3, 3), (HOP2, 6, 1), (PASS, 1, 0), (AGEND, 0, 0), (FWD, 0, 0),
        (ZEND, 0, 0), (PLACE, 7, 0), (ZUP, 7, 3), (ZUP, 7, 2), (ZUP, 7, 1), (PLACE, 6, 0),
        (ZUP, 6, 3), (ZUP, 6, 2), (ZUP, 6, 1), (FWD, 1, 0), (PASS, 0, 0), (ZEND, 2, 0),
        (BWD, 0, 0), (ZEND, 3, 0), (PASS, 2, 0), (ZEND, 4, 0), (BWD, 1, 0), (PASS, 3, 0),
        (ZEND, 5, 0), (G0, 0, 0), (PASS, 4, 0), (GSTEP, 0, 0), (ZEND, 7, 0), (PASS, 5, 0),
        (GSTEP, 1, 0), (ZEND, 6, 0), (PASS, 7, 0), (GSTEP, 2, 0), (PASS, 6, 0), (GEND, 0, 0),
    ),
    (
        (OWN, 0, 0), (OWN, 1, 0), (OWN, 2, 0), (OWN, 3, 0), (OWNP, 0, 0), (SQ, 0, 0),
        (TERM, 0, 0), (TERM, 1, 0), (SUM, 0, 0), (SUM, 1, 0), (AGZ, 0, 0), (AGZ, 2, 0),
        (AGSIDE, 0, 0), (AGSIDE, 2, 0), (SUM, 2, 0), (SUM, 3, 0), (SUM, 4, 0), (SUM, 5, 0),
        (SUM, 6, 0), (HOP1, 0, 0), (HOP1, 1, 0), (HOP1, 3, 0), (HOP1, 5, 0), (SUM, 7, 0),
        (HOP1, 7, 0), (SUM, 0, 1), (SUM, 1, 1), (SUM, 2, 1), (HOP1, 0, 1), (HOP1, 1, 1),
        (SUM, 3, 1), (SUM, 4, 1), (AGZ, 0, 1), (AGZ, 2, 1), (SUM, 5, 1), (SUM, 6, 1),
        (SUM, 7, 1), (AGSIDE, 0, 1), (HOP1, 3, 1), (AGPART, 0, 0), (HOP1, 5, 1), (AGZ, 0, 2),
        (AGZ, 2, 2), (AGSIDE, 2, 1), (AGPART, 2, 0), (AGSIDE, 0, 2), (AGZ, 0, 3), (AGZ, 2, 3),
        (HOP1, 2, 0), (AGSIDE, 2, 2), (HOP1, 2, 1), (AGZ, 3, 0), (AGSIDE, 3, 0), (AGSIDE, 0, 3),
        (AGPART, 0, 1), (AGZ, 3, 1), (AGSIDE, 3, 1), (AGSIDE, 2, 3), (AGPART, 2, 1), (AGPART, 0, 2),
        (AGZ, 3, 2), (HOP2, 1, 0), (AGSIDE, 3, 2), (HOP2, 1, 1), (AGPART, 2, 2), (AGZ, 3, 3),
        (HOP1, 4, 0), (AGSIDE, 3, 3), (HOP1, 4, 1), (AGPART, 3, 0), (AGPART, 0, 3), (HOP2, 3, 0),
        (HOP2, 0, 0), (HOP2, 3, 1), (AGPART, 3, 1), (HOP2, 0, 1), (AGPART, 2, 3), (HOP1, 6, 0),
        (HOP2, 2, 0), (PLACE, 1, 0), (ZUP, 1, 3), (HOP2, 2, 1), (HOP1, 6, 1), (ZUP, 1, 2),
        (HOP1, 7, 1), (AGPART, 3, 2), (ZDN, 1, 0), (HOP2, 5, 0), (ZEND, 1, 0), (HOP2, 4, 0),
        (HOP2, 5, 1), (AGPART, 3, 3), (HOP2, 4, 1), (HOP2, 7, 0), (AGEND, 0, 0), (FWD, 0, 0),
        (FWD, 1, 0), (PLACE, 0, 0), (ZUP, 0, 3), (ZUP, 0, 2), (PLACE, 2, 0), (ZUP, 2, 3),
        (ZUP, 2, 2), (PLACE, 3, 0), (ZUP, 3, 3), (ZUP, 3, 2), (BWD, 0, 0), (PASS, 1, 0),
        (ZDN, 0, 0), (BWD, 1, 0), (ZDN, 2, 0), (G0, 0, 0), (PLACE, 4, 0), (ZDN, 3, 0),
        (ZUP, 4, 3), (ZUP, 4, 2), (PLACE, 5, 0), (ZUP, 5, 3), (ZUP, 5, 2), (ZEND, 0, 0),
        (ZEND, 2, 0), (GSTEP, 0, 0), (HOP2, 6, 0), (HOP2, 6, 1), (HOP2, 7, 1), (ZEND, 3, 0),
        (ZDN, 4, 0), (PASS, 0, 0), (ZEND, 4, 0), (PASS, 2, 0), (GSTEP, 1, 0), (ZDN, 5, 0),
        (ZEND, 5, 0), (PLACE, 7, 0), (ZUP, 7, 3), (ZUP, 7, 2), (PLACE, 6, 0), (ZUP, 6, 3),
        (ZUP, 6, 2), (PASS, 3, 0), (PASS, 4, 0), (ZDN, 7, 0), (ZEND, 7, 0), (ZDN, 6, 0),
        (GSTEP, 2, 0), (ZEND, 6, 0), (PASS, 5, 0), (PASS, 7, 0), (PASS, 6, 0), (GEND, 0, 0),
    ),
)


def mirror(order, planes):
    flip = {ZUP: ZDN, ZDN: ZUP}
    out = []
    for step, a, b in order:
        if step in (ZUP, ZDN):
            b = planes - 1 - b
        if step in (AGZ, AGSIDE, AGPART):
            a = planes - 1 - a
        out.append((flip.get(step, step), a, b))
    return out


def plain_order(z, planes, cap):
    half = cap // 2
    out = [(OWN, k, 0) for k in range(half)] + [(OWNP, 0, 0), (SQ, 0, 0)]
    out += [(TERM, i, 0) for i in range(NI)]
    for step in (SUM, HOP1, HOP2):
        out += [(step, j, i) for j in range(NJ) for i in range(NI)]
    out += [(PLACE, j, 0) for j in range(NJ)]
    for step in (AGZ, AGSIDE, AGPART):
        for t in range(1, planes):
            for q in (z - t, z + t):
                if 0 <= q < planes:
                    out += [(step, q, k) for k in range(half)]
    for t in range(planes - 1):
        for j in range(NJ):
            if z < planes - 1 - t:
                out.append((ZUP, j, planes - 1 - t))
            if z > t:
                out.append((ZDN, j, t))
    for step in (ZEND, PASS):
        out += [(step, j, 0) for j in range(NJ)]
    out.append((AGEND, 0, 0))
    for step in (FWD, BWD):
        out += [(step, g, 0) for g in range(COMPUTE)]
    out.append((G0, 0, 0))
    out += [(GSTEP, n, 0) for n in range(3)]
    out.append((GEND, 0, 0))
    return out


def order_of(z, planes, cap):
    if planes == 4 and cap == 8:
        return list(TUNED[z]) if z < 2 else mirror(TUNED[planes - 1 - z], planes)
    return plain_order(z, planes, cap)


def split(order):
    parts, common = [[]], []
    for tok in order:
        if tok[0] in COMMON:
            common.append(tok)
            parts.append([])
        else:
            parts[-1].append(tok)
    return parts, common


def comm_kernel(
    planes, cap, nblk, scale,
    tok_h, gain_h, cot_h, bias_h, w_h, slot_of,
    proj, tgrad, frecv, vec,
    whole, tok, cot, gain, bias, inv, coef, fwd, gst, grecv, gz,
    part, drecv, r1, r2, slots, zup, zdn, bos,
    in_sem, agz_s, agz_r, ags_s, ags_r, agp_s, agp_r, own_s, own_r,
    d_s, d_r, r1_s, r1_r, r2_s, r2_r, zu_s, zu_r, zd_s, zd_r,
    f_s, f_r, p_s, p_r, g_s, g_r, gz_s, gz_r,
):
    s = lax.axis_index("shard")
    r = lax.axis_index("rep")
    z = s // 2
    c = s % 2
    quad = r % QUAD
    base = r - quad
    y = quad // 2
    x = quad % 2
    xq = y * 2 + (1 - x)
    yq = (1 - y) * 2 + x
    dq = (1 - y) * 2 + (1 - x)
    oc = 1 - c
    partner = (2 * z + oc, r)
    xdev = (s, base + xq)
    ydev = (s, base + yq)
    updev = (s + 2, r)
    dndev = (s - 2, r)
    near = [partner] + [(2 * z + cc, base + q) for q in (xq, yq) for cc in (c, oc)]
    others = [(2 * ((z + d) % planes) + c, r) for d in range(1, planes)]

    bar = pltpu.get_barrier_semaphore()
    for dev in near + others:
        pl.semaphore_signal(bar, inc=1, device_id=dev, device_id_type=MESH)

    loads = [
        pltpu.make_async_copy(w_h, whole.at[pl.ds(s * cap, cap)], in_sem.at[0]),
        pltpu.make_async_copy(tok_h, tok, in_sem.at[1]),
        pltpu.make_async_copy(cot_h, cot, in_sem.at[2]),
        pltpu.make_async_copy(gain_h, gain, in_sem.at[3]),
        pltpu.make_async_copy(bias_h, bias, in_sem.at[4]),
    ]
    for cp in loads:
        cp.start()

    def owner(u, carry):
        found = jnp.int32(-1)
        for b in range(nblk):
            found = jnp.where(slot_of[b] == u, b, found)
        bos[u] = found
        return carry

    lax.fori_loop(0, 2 * planes * cap, owner, 0)
    loads[0].wait()
    pl.semaphore_wait(bar, len(near) + len(others))

    def rdma(src, dst, ss, rs, dev):
        return pltpu.make_async_remote_copy(
            src_ref=src, dst_ref=dst, send_sem=ss, recv_sem=rs, device_id=dev, device_id_type=MESH
        )

    half = cap // 2
    quar = cap // 4
    hh = (x + y) % 2
    tokens_here, width = tok.shape
    wide = 4 * BLK
    nb = nblk // NI
    per_plane = 2 * cap

    def held(q, core, which, k):
        start = hh * half if which == 0 else (1 - hh) * half
        return whole.at[pl.ds((2 * q + core) * cap + start + k, 1)]

    def ag_z(q, d, k):
        ref = held(q, c, 0, k)
        return rdma(ref, ref, agz_s.at[d, q, k], agz_r.at[q, k], updev if d == 0 else dndev)

    def ag_side(q, which, k):
        ref = held(q, c, which, k)
        return rdma(ref, ref, ags_s.at[q, k], ags_r.at[q, k], xdev if k < quar else ydev)

    def ag_part(q, core, which, k):
        ref = held(q, core, which, k)
        return rdma(ref, ref, agp_s.at[which, q, k], agp_r.at[which, q, k], partner)

    def own_part(core):
        ref = whole.at[pl.ds((2 * z + core) * cap, cap)]
        return rdma(ref, ref, own_s, own_r, partner)

    def onward(zz, q):
        out = []
        if q <= zz < planes - 1:
            out.append(0)
        if q >= zz > 0:
            out.append(1)
        return out

    def d_copy(j, i):
        blocks = pl.ds(i * nb, nb)
        return rdma(
            part.at[oc, j, :, blocks], drecv.at[j, :, blocks], d_s.at[j, i], d_r.at[j, i], partner
        )

    def first_hop(j, i, n):
        q, dev = (xq, xdev) if j % 2 == 0 else (yq, ydev)
        q = (q, dq)[n]
        blocks = pl.ds(i * nb, nb)
        return rdma(
            part.at[c, j, q, blocks], r1.at[j, n, blocks], r1_s.at[j, i, n], r1_r.at[j, i, n], dev
        )

    def second_hop(j, i):
        far, dev = (yq, ydev) if j % 2 == 0 else (xq, xdev)
        blocks = pl.ds(i * nb, nb)
        return rdma(
            part.at[c, j, far, blocks], r2.at[j, blocks], r2_s.at[j, i], r2_r.at[j, i], dev
        )

    def add_to(dst, src, start, count):
        step = next(n for n in (10, 8, 5, 4, 2, 1) if count % n == 0)

        def body(i, carry):
            sl = pl.ds(start + i * step, step)
            dst[sl] = (dst[sl].astype(F32) + src[sl].astype(F32)).astype(BF16)
            return carry

        lax.fori_loop(0, count // step, body, 0)

    def z_copy(j, q, up):
        if up:
            return rdma(slots.at[j, q], zup.at[j, q], zu_s.at[j, q], zu_r.at[j, q], updev)
        return rdma(slots.at[j, q], zdn.at[j, q], zd_s.at[j, q], zd_r.at[j, q], dndev)

    my_id = quad * 2 + c

    def f_copies(zz, j):
        out = []
        for n, dev in enumerate(near):
            cc = oc if n in (0, 2, 4) else c
            out.append(
                rdma(
                    slots.at[j, zz, pl.ds(cc * cap, cap)], frecv.at[j, my_id],
                    f_s.at[j, n], f_r.at[j, my_id], dev,
                )
            )
        return out

    def f_got(j, q, core):
        sender = q * 2 + core
        return rdma(
            slots.at[j, 0, pl.ds(0, cap)], frecv.at[j, sender], f_s.at[j, 0], f_r.at[j, sender], partner
        )

    def f_pass(j):
        q, dev = (xq, ydev) if j % 2 == 0 else (yq, xdev)
        pair = frecv.at[j, pl.ds(q * 2, 2)]
        return rdma(pair, pair, p_s.at[j], p_r.at[j], dev)

    def f_passed(j):
        pair = frecv.at[j, pl.ds(dq * 2, 2)]
        return rdma(pair, pair, p_s.at[j], p_r.at[j], ydev if j % 2 == 0 else xdev)

    def g_copy(n):
        dev = (partner, xdev, ydev)[n]
        return rdma(gst.at[n], grecv.at[n], g_s.at[n], g_r.at[n], dev)

    def gz_copy(d, q):
        return rdma(gst.at[3], gz.at[q], gz_s.at[d - 1], gz_r.at[q], others[d - 1])

    def squares(i, acc):
        v = tok[:, pl.ds(pl.multiple_of(i * 2 * BLK, 2 * BLK), 2 * BLK)].astype(F32)
        v = v * v
        return acc + v[:, :BLK] + v[:, BLK:]

    def term(i, carry):
        cols = pl.ds(pl.multiple_of(i * wide, wide), wide)
        normed = (tok[:, cols].astype(F32) * inv[...] * gain[:, cols]).astype(BF16)
        res = lax.dot_general(
            normed, cot[...], (((0,), (0,)), ((), ())), preferred_element_type=F32
        )
        res = (res * scale).astype(BF16)
        group = res.shape[1] // (2 * QUAD)
        for b in range(wide // BLK):
            for j in range(NJ):
                lo = b * BLK + j * SUB
                for k in range(QUAD):
                    for cc in range(2):
                        col = (k * 2 + cc) * group
                        part[cc, j, k, i * (wide // BLK) + b] = res[lo:lo + SUB, col:col + group]
        return carry

    grp = 4
    gw = grp * BLK
    groups = nblk // grp
    cuts = [groups * i // COMPUTE for i in range(COMPUTE + 1)]

    def weight_group(g):
        return jnp.concatenate([whole[slot_of[g * grp + i]] for i in range(grp)], axis=0)

    def fwd_body(g, carry):
        cols = pl.ds(pl.multiple_of(g * gw, gw), gw)
        normed = (tok[:, cols].astype(F32) * inv[...] * gain[:, cols]).astype(BF16)
        fwd[...] += jnp.dot(normed, weight_group(g), preferred_element_type=F32)
        return carry

    def bwd_body(g, carry):
        cols = pl.ds(pl.multiple_of(g * gw, gw), gw)
        grad = lax.dot_general(
            cot[...], weight_group(g), (((1,), (1,)), ((), ())), preferred_element_type=F32
        )
        values = tok[:, cols].astype(F32)
        tgrad[:, cols] = (grad * gain[:, cols] * inv[...] - values * coef[...]).astype(BF16)
        gst[0, :, cols] = jnp.sum(grad * values * inv[...], axis=0, keepdims=True) * scale
        return carry

    def shared_step(step, a):
        if step == SQ:
            loads[1].wait()
            acc = lax.fori_loop(
                0, width // (2 * BLK), squares, jnp.zeros((tokens_here, BLK), F32)
            )
            inv[...] = lax.rsqrt(jnp.sum(acc, axis=1, keepdims=True) / width + EPS)
            for cp in loads[2:]:
                cp.wait()
        elif step == TERM:
            count = width // wide
            lax.fori_loop(a * count // NI, (a + 1) * count // NI, term, 0)
            for j in range(NJ):
                d_copy(j, a).start()
        elif step == FWD:
            if a == 0:
                fwd[...] = jnp.zeros_like(fwd)
            lax.fori_loop(cuts[a], cuts[a + 1], fwd_body, 0)
        else:
            if a == 0:
                total = fwd[...]
                proj[...] = (total + bias[...]).astype(BF16)
                inner = jnp.sum(total * cot[...].astype(F32), axis=1, keepdims=True) / width
                coef[...] = inv[...] * inv[...] * inner
                gst[0, :, width:] = jnp.sum(cot[...].astype(F32), axis=0, keepdims=True) * scale
            lax.fori_loop(cuts[a], cuts[a + 1], bwd_body, 0)

    def own_step(zz, step, a, b):
        if step == OWN:
            for d in onward(zz, zz):
                ag_z(zz, d, a).start()
        elif step == OWNP:
            own_part(c).start()
        elif step == AGZ:
            ag_z(a, 0, b).wait_recv()
            for d in onward(zz, a):
                ag_z(a, d, b).start()
            ag_part(a, c, 0, b).start()
        elif step == AGSIDE:
            ag_side(a, 0, b).start()
        elif step == AGPART:
            ag_side(a, 1, b).wait_recv()
            ag_part(a, c, 1, b).start()
        elif step == AGEND:
            for q in range(planes):
                if q != zz:
                    for k in range(half):
                        ag_part(q, oc, 0, k).wait_recv()
                        ag_part(q, oc, 1, k).wait_recv()
            own_part(oc).wait_recv()
        elif step == SUM:
            d_copy(a, b).wait()
            for k in range(QUAD):
                add_to(part.at[c, a, k], drecv.at[a, k], b * nb, nb)
        elif step == HOP1:
            first_hop(a, b, 1).start()
            first_hop(a, b, 0).start()
        elif step == HOP2:
            far = yq if a % 2 == 0 else xq
            first_hop(a, b, 1).wait_recv()
            add_to(part.at[c, a, far], r1.at[a, 1], b * nb, nb)
            second_hop(a, b).start()
            first_hop(a, b, 0).wait_recv()
            add_to(part.at[c, a, quad], r1.at[a, 0], b * nb, nb)
        elif step == PLACE:
            for i in range(NI):
                second_hop(a, i).wait_recv()
            add_to(part.at[c, a, quad], r2.at[a], 0, nblk)

            def body(i, carry):
                for u in range(per_plane):
                    k = bos[i * per_plane + u]
                    val = part[c, a, quad, jnp.maximum(k, 0)]
                    slots[a, i, u] = jnp.where(k >= 0, val.astype(F32), 0.0).astype(BF16)
                return carry

            lax.fori_loop(0, planes, body, 0)
        elif step == ZUP:
            if zz > 0:
                z_copy(a, b, True).wait_recv()
                add_to(slots.at[a, b], zup.at[a, b], 0, per_plane)
            z_copy(a, b, True).start()
        elif step == ZDN:
            if zz < planes - 1:
                z_copy(a, b, False).wait_recv()
                add_to(slots.at[a, b], zdn.at[a, b], 0, per_plane)
            z_copy(a, b, False).start()
        elif step == ZEND:
            if zz > 0:
                z_copy(a, zz, True).wait_recv()
                add_to(slots.at[a, zz], zup.at[a, zz], 0, per_plane)
            if zz < planes - 1:
                z_copy(a, zz, False).wait_recv()
                add_to(slots.at[a, zz], zdn.at[a, zz], 0, per_plane)
            for cp in f_copies(zz, a):
                cp.start()
            frecv[a, my_id] = slots[a, zz, pl.ds(c * cap, cap)]
        elif step == PASS:
            q = xq if a % 2 == 0 else yq
            f_got(a, q, 0).wait_recv()
            f_got(a, q, 1).wait_recv()
            f_pass(a).start()
        elif step == G0:
            g_copy(0).start()
        elif step == GSTEP:
            g_copy(a).wait_recv()
            gst[a + 1] = gst[a] + grecv[a]
            if a < 2:
                g_copy(a + 1).start()
            else:
                gz[zz] = gst[3]
                for d in range(1, planes):
                    gz_copy(d, zz).start()
        elif step == GEND:
            for d in range(1, planes):
                gz_copy(d, (zz + d) % planes).wait_recv()
            total = gz[0]
            for q in range(1, planes):
                total = total + gz[q]
            vec[...] = total

    def finish(zz):
        for j in range(NJ):
            f_got(j, quad, oc).wait_recv()
            q = yq if j % 2 == 0 else xq
            f_got(j, q, 0).wait_recv()
            f_got(j, q, 1).wait_recv()
            f_passed(j).wait_recv()
        for q in range(planes):
            for k in range(half):
                for d in onward(zz, q):
                    ag_z(q, d, k).wait_send()
                if q != zz:
                    ag_side(q, 0, k).wait_send()
                    ag_part(q, c, 0, k).wait_send()
                    ag_part(q, c, 1, k).wait_send()
        own_part(c).wait_send()
        for j in range(NJ):
            for i in range(NI):
                first_hop(j, i, 0).wait_send()
                first_hop(j, i, 1).wait_send()
                second_hop(j, i).wait_send()
            for q in range(planes):
                if q > zz:
                    z_copy(j, q, True).wait_send()
                if q < zz:
                    z_copy(j, q, False).wait_send()
            for cp in f_copies(zz, j):
                cp.wait_send()
            f_pass(j).wait_send()
        for n in range(3):
            g_copy(n).wait_send()
        for d in range(1, planes):
            gz_copy(d, zz).wait_send()

    plans = [split(order_of(zz, planes, cap)) for zz in range(planes)]
    common = plans[0][1]
    for n in range(len(common) + 1):
        for zz in range(planes):
            assert plans[zz][1] == common
            todo = plans[zz][0][n]
            last = n == len(common)
            if todo or last:
                @pl.when(z == zz)
                def _():
                    for tk in todo:
                        own_step(zz, *tk)
                    if last:
                        finish(zz)

        if n < len(common):
            shared_step(*common[n][:2])


def write_kernel(proj, tgrad, frecv, vec, proj_h, tgrad_h, wgrad_h, gain_h, bias_h, buf, sem, wsem):
    width = gain_h.shape[1]
    cap = frecv.shape[2]
    copies = [
        pltpu.make_async_copy(tgrad, tgrad_h, sem.at[0]),
        pltpu.make_async_copy(proj, proj_h, sem.at[1]),
        pltpu.make_async_copy(vec.at[:, :width], gain_h, sem.at[2]),
        pltpu.make_async_copy(vec.at[:, width:], bias_h, sem.at[3]),
    ]
    for cp in copies:
        cp.start()
    for u in range(cap):
        for j in range(NJ):
            for n in range(2 * QUAD):
                buf[u, j * SUB:(j + 1) * SUB, n * BLK:(n + 1) * BLK] = frecv[j, n, u].astype(F32)
        cp = pltpu.make_async_copy(buf.at[u], wgrad_h.at[u], wsem.at[u])
        cp.start()
        copies.append(cp)
    for cp in copies:
        cp.wait()


def communicate(tokens, norm_gain, cotangent, key_bias, block_slot, key_weight, scale):
    shard_count = lax.axis_size("shard")
    planes = shard_count // 2
    rows, cols = key_weight.shape
    cap = rows // BLK
    half = cap // 2
    tok_count, width = tokens.shape
    nblk = width // BLK
    group = cols // (2 * QUAD)
    dma = pltpu.SemaphoreType.DMA
    vm = pltpu.VMEM
    hbm = pl.BlockSpec(memory_space=pl.ANY)
    local = pl.BlockSpec(memory_space=vm)
    held = pl.pallas_call(
        functools.partial(comm_kernel, planes, cap, nblk, scale),
        out_shape=(
            vm((tok_count, cols), BF16),
            vm((tok_count, width), BF16),
            vm((NJ, 2 * QUAD, cap, SUB, group), BF16),
            vm((1, width + cols), F32),
        ),
        in_specs=[hbm, hbm, hbm, hbm, hbm, pl.BlockSpec(memory_space=pltpu.SMEM)],
        out_specs=(local,) * 4,
        scratch_shapes=[
            vm((shard_count * cap, BLK, cols), BF16),
            vm((tok_count, width), BF16),
            vm((tok_count, cols), BF16),
            vm((1, width), F32),
            vm((1, cols), F32),
            vm((tok_count, 1), F32),
            vm((tok_count, 1), F32),
            vm((tok_count, cols), F32),
            vm((4, 1, width + cols), F32),
            vm((3, 1, width + cols), F32),
            vm((planes, 1, width + cols), F32),
            vm((2, NJ, QUAD, nblk, SUB, group), BF16),
            vm((NJ, QUAD, nblk, SUB, group), BF16),
            vm((NJ, 2, nblk, SUB, group), BF16),
            vm((NJ, nblk, SUB, group), BF16),
            vm((NJ, planes, 2 * cap, SUB, group), BF16),
            vm((NJ, planes, 2 * cap, SUB, group), BF16),
            vm((NJ, planes, 2 * cap, SUB, group), BF16),
            pltpu.SMEM((shard_count * cap,), jnp.int32),
            dma((5,)),
            dma((2, planes, half)), dma((planes, half)),
            dma((planes, half)), dma((planes, half)),
            dma((2, planes, half)), dma((2, planes, half)),
            dma(()), dma(()),
            dma((NJ, NI)), dma((NJ, NI)),
            dma((NJ, NI, 2)), dma((NJ, NI, 2)),
            dma((NJ, NI)), dma((NJ, NI)),
            dma((NJ, planes)), dma((NJ, planes)),
            dma((NJ, planes)), dma((NJ, planes)),
            dma((NJ, 5)), dma((NJ, 8)),
            dma((NJ,)), dma((NJ,)),
            dma((3,)), dma((3,)),
            dma((planes,)), dma((planes,)),
        ],
        compiler_params=pltpu.CompilerParams(
            collective_id=0, has_side_effects=True, vmem_limit_bytes=54 * 2**20
        ),
    )(
        tokens, norm_gain[None, :], cotangent, key_bias[None, :],
        key_weight.reshape(cap, BLK, cols), block_slot,
    )
    return pl.pallas_call(
        write_kernel,
        out_shape=(
            jax.ShapeDtypeStruct((tok_count, cols), BF16),
            jax.ShapeDtypeStruct((tok_count, width), BF16),
            jax.ShapeDtypeStruct((cap, BLK, cols), F32),
            jax.ShapeDtypeStruct((1, width), F32),
            jax.ShapeDtypeStruct((1, cols), F32),
        ),
        in_specs=[local] * 4,
        out_specs=(hbm,) * 5,
        scratch_shapes=[vm((cap, BLK, cols), F32), dma((4,)), dma((cap,))],
        compiler_params=pltpu.CompilerParams(vmem_limit_bytes=8 * 2**20),
    )(*held)


def local(tokens, norm_gain, key_bias, key_weight, cotangent, block_slot):
    row_count, width = tokens.shape
    shard_count = lax.axis_size("shard")
    replicas = lax.axis_size("rep")
    grad_scale = float(row_count * shard_count * replicas) ** (-0.5)
    projected, token_grad, weight_grad, gain_grad, bias_grad = communicate(
        tokens, norm_gain, cotangent, key_bias, block_slot, key_weight, grad_scale
    )
    weight_grad = weight_grad.reshape(key_weight.shape)
    if replicas > QUAD:
        groups = [list(range(i, replicas, QUAD)) for i in range(QUAD)]
        weight_grad, gain_grad, bias_grad = lax.psum(
            (weight_grad, gain_grad, bias_grad), "rep", axis_index_groups=groups
        )
    return (projected, token_grad, weight_grad, gain_grad[0], bias_grad[0])


def solution(mesh):
    return jax.shard_map(
        local,
        mesh=mesh,
        in_specs=(
            P(("shard", "rep"), None),
            P(),
            P(),
            P("shard", None),
            P(("shard", "rep"), None),
            P(),
        ),
        out_specs=(
            P(("shard", "rep"), None),
            P(("shard", "rep"), None),
            P("shard", None),
            P(),
            P(),
        ),
        check_vma=False,
    )
```

```python
import functools
import jax
import jax.numpy as jnp
from jax import lax
from jax.experimental import pallas as pl
from jax.experimental.pallas import tpu as pltpu
from jax.sharding import PartitionSpec as P

BLK = 128
EPS = 1e-06
NJ = 8
NI = 4
SUB = BLK // NJ
QUAD = 4
MESH = pl.DeviceIdType.MESH
F32 = jnp.float32
BF16 = jnp.bfloat16
COMPUTE = 3
FGRP = 8
BGRP = 4

OWN, OWNP, SQ, TERM, SUM, HOP1, HOP2, PLACE, ZUP, ZDN, ZEND, PASS = range(12)
FWD, BWD, AGZ, AGSIDE, AGPART, AGEND, G0, GSTEP, GEND, OWNER = range(12, 22)
COMMON = (SQ, TERM, FWD, BWD)

TUNED = (
    (
        (OWN, 0, 0), (OWN, 1, 0), (OWN, 2, 0), (OWN, 3, 0), (OWNP, 0, 0), (SQ, 0, 0), (TERM, 0, 0),
        (TERM, 1, 0), (SUM, 0, 0), (HOP1, 0, 0), (SUM, 1, 0), (HOP1, 1, 0), (SUM, 3, 0), (SUM, 2, 0),
        (SUM, 5, 0), (HOP1, 5, 0), (HOP1, 3, 0), (HOP1, 2, 0), (TERM, 2, 0), (AGZ, 1, 0), (AGSIDE, 1, 0),
        (SUM, 4, 1), (SUM, 1, 1), (HOP2, 2, 0), (SUM, 1, 2), (HOP1, 1, 1), (SUM, 3, 1), (HOP1, 3, 1),
        (SUM, 4, 0), (SUM, 5, 1), (TERM, 3, 0), (HOP1, 4, 1), (SUM, 7, 2), (HOP1, 5, 1), (HOP1, 7, 2),
        (SUM, 0, 3), (SUM, 3, 2), (SUM, 0, 1), (HOP2, 0, 0), (SUM, 3, 3), (HOP1, 0, 3), (SUM, 2, 1),
        (SUM, 5, 3), (AGZ, 1, 1), (SUM, 0, 2), (SUM, 2, 2), (SUM, 4, 3), (HOP2, 5, 0), (SUM, 6, 1),
        (HOP2, 1, 0), (HOP1, 3, 3), (HOP1, 0, 1), (SUM, 1, 3), (SUM, 5, 2), (HOP1, 1, 3), (HOP1, 2, 1),
        (HOP1, 4, 0), (HOP1, 4, 3), (HOP1, 3, 2), (SUM, 2, 3), (HOP1, 0, 2), (HOP1, 5, 3), (HOP2, 2, 1),
        (SUM, 4, 2), (HOP2, 4, 0), (HOP1, 2, 2), (AGPART, 1, 0), (HOP2, 0, 1), (AGZ, 1, 2), (HOP1, 1, 2),
        (HOP2, 3, 1), (HOP2, 3, 0), (HOP1, 2, 3), (HOP2, 0, 3), (AGSIDE, 1, 2), (SUM, 6, 2), (HOP1, 4, 2),
        (AGSIDE, 1, 1), (HOP2, 3, 3), (SUM, 7, 3), (HOP2, 1, 1), (SUM, 6, 3), (HOP2, 1, 2), (HOP2, 4, 1),
        (HOP2, 1, 3), (OWNER, 0, 0), (SUM, 7, 0), (HOP2, 5, 3), (AGZ, 2, 0), (HOP2, 2, 3), (HOP2, 0, 2),
        (HOP2, 3, 2), (AGSIDE, 2, 0), (AGZ, 1, 3), (HOP2, 4, 3), (HOP2, 4, 2), (AGSIDE, 1, 3), (HOP2, 2, 2),
        (SUM, 7, 1), (SUM, 6, 0), (PLACE, 0, 0), (HOP1, 7, 3), (PLACE, 1, 0), (ZUP, 0, 2), (AGZ, 2, 1),
        (PLACE, 3, 0), (AGZ, 2, 2), (AGSIDE, 2, 1), (AGPART, 1, 3), (HOP1, 6, 0), (PLACE, 4, 0), (ZUP, 1, 2),
        (ZUP, 0, 3), (AGSIDE, 2, 2), (HOP1, 5, 2), (AGZ, 2, 3), (PLACE, 2, 0), (ZUP, 4, 1), (AGSIDE, 2, 3),
        (AGZ, 3, 0), (AGSIDE, 3, 0), (ZUP, 1, 3), (HOP2, 5, 2), (ZUP, 2, 2), (HOP1, 6, 3), (AGZ, 3, 2),
        (ZUP, 3, 3), (AGSIDE, 3, 2), (ZUP, 4, 3), (HOP1, 7, 1), (ZUP, 3, 1), (AGPART, 1, 1), (AGPART, 2, 0),
        (AGZ, 3, 1), (HOP2, 5, 1), (AGSIDE, 3, 1), (ZUP, 2, 3), (AGPART, 1, 2), (AGZ, 3, 3), (ZUP, 3, 2),
        (HOP1, 6, 1), (AGSIDE, 3, 3), (HOP1, 7, 0), (AGPART, 3, 2), (HOP2, 6, 3), (HOP2, 6, 0), (PLACE, 5, 0),
        (ZUP, 4, 2), (AGPART, 2, 2), (HOP1, 6, 2), (ZUP, 5, 1), (ZUP, 5, 3), (ZUP, 0, 1), (ZUP, 1, 1),
        (HOP2, 7, 3), (AGPART, 3, 0), (AGPART, 2, 3), (AGPART, 3, 1), (ZUP, 2, 1), (AGPART, 2, 1), (HOP2, 6, 1),
        (AGPART, 3, 3), (HOP2, 7, 1), (HOP2, 7, 2), (ZUP, 5, 2), (HOP2, 6, 2), (HOP2, 7, 0), (AGEND, 0, 0),
        (FWD, 0, 0), (ZEND, 1, 0), (FWD, 1, 0), (ZEND, 2, 0), (PLACE, 6, 0), (ZUP, 6, 3), (PLACE, 7, 0),
        (ZUP, 7, 3), (ZUP, 6, 2), (ZUP, 7, 1), (ZEND, 3, 0), (FWD, 2, 0), (ZUP, 7, 2), (PASS, 1, 0),
        (BWD, 0, 0), (PASS, 2, 0), (ZEND, 4, 0), (ZEND, 0, 0), (ZUP, 6, 1), (BWD, 1, 0), (ZEND, 5, 0),
        (BWD, 2, 0), (G0, 0, 0), (GSTEP, 0, 0), (ZEND, 6, 0), (PASS, 5, 0), (ZEND, 7, 0), (PASS, 4, 0),
        (PASS, 3, 0), (GSTEP, 1, 0), (PASS, 6, 0), (PASS, 0, 0), (PASS, 7, 0), (GEND, 0, 0),
    ),
    (
        (OWN, 0, 0), (OWN, 1, 0), (OWN, 2, 0), (OWN, 3, 0), (OWNP, 0, 0), (SQ, 0, 0), (TERM, 0, 0),
        (TERM, 1, 0), (SUM, 0, 0), (SUM, 3, 0), (SUM, 2, 0), (HOP1, 2, 0), (SUM, 1, 0), (HOP1, 3, 0),
        (HOP1, 1, 0), (HOP1, 0, 0), (TERM, 2, 0), (SUM, 1, 1), (HOP1, 1, 1), (SUM, 0, 1), (SUM, 3, 1),
        (AGZ, 2, 0), (SUM, 4, 1), (AGSIDE, 2, 0), (HOP2, 0, 0), (SUM, 7, 1), (SUM, 3, 2), (SUM, 1, 2),
        (HOP1, 4, 1), (HOP1, 1, 2), (AGZ, 0, 0), (HOP1, 7, 1), (SUM, 6, 1), (AGSIDE, 0, 0), (SUM, 5, 2),
        (AGZ, 2, 1), (HOP1, 3, 1), (HOP2, 4, 1), (HOP1, 3, 2), (SUM, 0, 2), (AGZ, 2, 2), (AGSIDE, 2, 2),
        (TERM, 3, 0), (AGSIDE, 2, 1), (AGZ, 2, 3), (SUM, 0, 3), (HOP1, 0, 3), (HOP2, 1, 0), (AGZ, 0, 1),
        (HOP1, 0, 2), (SUM, 1, 3), (HOP1, 1, 3), (AGZ, 0, 2), (AGSIDE, 0, 2), (AGZ, 0, 3), (AGSIDE, 0, 1),
        (SUM, 2, 1), (AGSIDE, 0, 3), (HOP2, 3, 2), (SUM, 7, 0), (SUM, 7, 3), (HOP2, 1, 3), (AGPART, 2, 1),
        (HOP2, 1, 1), (SUM, 6, 0), (HOP1, 0, 1), (SUM, 4, 0), (AGZ, 3, 0), (HOP1, 7, 3), (SUM, 2, 3),
        (SUM, 6, 2), (SUM, 5, 0), (SUM, 5, 3), (HOP2, 0, 2), (HOP1, 6, 2), (HOP2, 0, 3), (SUM, 2, 2),
        (AGSIDE, 2, 3), (SUM, 7, 2), (AGZ, 3, 2), (AGPART, 0, 2), (SUM, 3, 3), (HOP2, 3, 1), (HOP2, 0, 1),
        (AGZ, 3, 1), (AGSIDE, 3, 0), (AGSIDE, 3, 1), (AGSIDE, 3, 2), (AGZ, 3, 3), (HOP2, 1, 2), (HOP1, 2, 2),
        (AGSIDE, 3, 3), (AGPART, 2, 0), (OWNER, 0, 0), (AGPART, 3, 2), (AGPART, 3, 0), (HOP2, 3, 0), (AGPART, 3, 1),
        (AGPART, 0, 1), (HOP1, 2, 3), (AGPART, 0, 0), (SUM, 4, 2), (AGPART, 0, 3), (PLACE, 1, 0), (HOP2, 2, 0),
        (HOP1, 2, 1), (ZUP, 1, 3), (HOP1, 3, 3), (SUM, 5, 1), (SUM, 4, 3), (AGPART, 3, 3), (HOP1, 4, 2),
        (PLACE, 0, 0), (HOP1, 5, 0), (AGPART, 2, 3), (HOP2, 2, 3), (HOP2, 2, 2), (HOP2, 7, 3), (HOP2, 3, 3),
        (HOP2, 2, 1), (HOP1, 5, 2), (HOP1, 4, 0), (ZUP, 0, 2), (SUM, 6, 3), (ZUP, 0, 3), (HOP1, 5, 3),
        (HOP1, 5, 1), (AGPART, 2, 2), (HOP1, 4, 3), (AGEND, 0, 0), (FWD, 0, 0), (HOP2, 4, 0), (HOP1, 6, 1),
        (ZUP, 1, 2), (PLACE, 3, 0), (ZUP, 3, 3), (HOP1, 6, 3), (HOP2, 4, 2), (FWD, 1, 0), (ZDN, 1, 0),
        (HOP2, 4, 3), (HOP2, 5, 0), (ZUP, 3, 2), (ZDN, 0, 0), (PLACE, 2, 0), (ZUP, 2, 3), (FWD, 2, 0),
        (HOP1, 7, 2), (HOP1, 7, 0), (HOP2, 5, 1), (HOP2, 6, 1), (HOP2, 6, 2), (HOP2, 5, 3), (ZDN, 3, 0),
        (HOP2, 5, 2), (BWD, 0, 0), (HOP2, 7, 1), (HOP2, 6, 3), (PLACE, 4, 0), (ZDN, 2, 0), (ZEND, 0, 0),
        (ZUP, 4, 3), (PLACE, 5, 0), (HOP1, 6, 0), (ZEND, 1, 0), (ZUP, 4, 2), (ZUP, 5, 3), (ZDN, 4, 0),
        (ZUP, 2, 2), (BWD, 1, 0), (HOP2, 7, 0), (ZUP, 5, 2), (HOP2, 7, 2), (HOP2, 6, 0), (ZEND, 3, 0),
        (ZDN, 5, 0), (ZEND, 4, 0), (BWD, 2, 0), (G0, 0, 0), (PLACE, 6, 0), (ZUP, 6, 3), (PASS, 1, 0),
        (PLACE, 7, 0), (ZEND, 5, 0), (ZUP, 7, 3), (ZUP, 6, 2), (PASS, 0, 0), (ZDN, 6, 0), (ZEND, 2, 0),
        (GSTEP, 0, 0), (PASS, 4, 0), (PASS, 3, 0), (ZUP, 7, 2), (ZDN, 7, 0), (ZEND, 6, 0), (PASS, 5, 0),
        (ZEND, 7, 0), (GSTEP, 1, 0), (PASS, 6, 0), (PASS, 7, 0), (PASS, 2, 0), (GEND, 0, 0),
    ),
)


def mirror(order, planes):
    flip = {ZUP: ZDN, ZDN: ZUP}
    out = []
    for step, a, b in order:
        if step in (ZUP, ZDN):
            b = planes - 1 - b
        if step in (AGZ, AGSIDE, AGPART):
            a = planes - 1 - a
        out.append((flip.get(step, step), a, b))
    return out


def plain_order(z, planes, cap):
    half = cap // 2
    out = [(OWN, k, 0) for k in range(half)] + [(OWNP, 0, 0), (SQ, 0, 0), (OWNER, 0, 0)]
    out += [(TERM, i, 0) for i in range(NI)]
    for step in (SUM, HOP1, HOP2):
        out += [(step, j, i) for j in range(NJ) for i in range(NI)]
    out += [(PLACE, j, 0) for j in range(NJ)]
    for step in (AGZ, AGSIDE, AGPART):
        for t in range(1, planes):
            for q in (z - t, z + t):
                if 0 <= q < planes:
                    out += [(step, q, k) for k in range(half)]
    for t in range(planes - 1):
        for j in range(NJ):
            if z < planes - 1 - t:
                out.append((ZUP, j, planes - 1 - t))
            if z > t:
                out.append((ZDN, j, t))
    for step in (ZEND, PASS):
        out += [(step, j, 0) for j in range(NJ)]
    out.append((AGEND, 0, 0))
    for step in (FWD, BWD):
        out += [(step, g, 0) for g in range(COMPUTE)]
    out.append((G0, 0, 0))
    out += [(GSTEP, n, 0) for n in range(2)]
    out.append((GEND, 0, 0))
    return out


def order_of(z, planes, cap):
    if planes == 4 and cap == 8:
        return list(TUNED[z]) if z < 2 else mirror(TUNED[planes - 1 - z], planes)
    return plain_order(z, planes, cap)


def split(order):
    parts, common = [[]], []
    for tok in order:
        if tok[0] in COMMON:
            common.append(tok)
            parts.append([])
        else:
            parts[-1].append(tok)
    return parts, common


def comm_kernel(
    planes, cap, nblk, scale,
    tok_h, gain_h, cot_h, bias_h, w_h, slot_of,
    proj, tgrad, frecv, vec,
    whole, tok, cot, gain, bias, inv, coef, fwd, gst, grecv, gz,
    part, drecv, r1, r2, slots, zup, zdn, bos,
    in_sem, agz_r, ags_r, agp_r, d_r, r1_r, r2_r, z_r, pass_r, end_r, g_r, gz_r, sent,
):
    s = lax.axis_index("shard")
    r = lax.axis_index("rep")
    z = s // 2
    c = s % 2
    quad = r % QUAD
    base = r - quad
    y = quad // 2
    x = quad % 2
    xq = y * 2 + (1 - x)
    yq = (1 - y) * 2 + x
    dq = (1 - y) * 2 + (1 - x)
    oc = 1 - c
    partner = (2 * z + oc, r)
    xdev = (s, base + xq)
    ydev = (s, base + yq)
    updev = (s + 2, r)
    dndev = (s - 2, r)
    ddev = (s, base + dq)
    near = [partner] + [(2 * z + cc, base + q) for q in (xq, yq) for cc in (c, oc)]
    others = [(2 * ((z + d) % planes) + c, r) for d in range(1, planes)]

    bar = pltpu.get_barrier_semaphore()
    greet = near + [ddev] + others
    for dev in greet:
        pl.semaphore_signal(bar, inc=1, device_id=dev, device_id_type=MESH)

    loads = [
        pltpu.make_async_copy(w_h, whole.at[pl.ds(s * cap, cap)], in_sem.at[0]),
        pltpu.make_async_copy(tok_h, tok, in_sem.at[1]),
        pltpu.make_async_copy(cot_h, cot, in_sem.at[2]),
        pltpu.make_async_copy(gain_h, gain, in_sem.at[3]),
        pltpu.make_async_copy(bias_h, bias, in_sem.at[4]),
    ]
    for cp in loads:
        cp.start()

    def owner(u, carry):
        found = jnp.int32(-1)
        for b in range(nblk):
            found = jnp.where(slot_of[b] == u, b, found)
        bos[u] = found
        return carry

    loads[0].wait()
    pl.semaphore_wait(bar, len(greet))

    def rdma(src, dst, ss, rs, dev):
        return pltpu.make_async_remote_copy(
            src_ref=src, dst_ref=dst, send_sem=ss, recv_sem=rs, device_id=dev, device_id_type=MESH
        )

    half = cap // 2
    quar = cap // 4
    hh = (x + y) % 2
    tokens_here, width = tok.shape
    wide = 5 * BLK
    nb = nblk // NI
    per_plane = 2 * cap

    def held(q, core, which, k):
        start = hh * half if which == 0 else (1 - hh) * half
        return whole.at[pl.ds((2 * q + core) * cap + start + k, 1)]

    def ag_z(q, d, k):
        ref = held(q, c, 0, k)
        return rdma(ref, ref, sent.at[0], agz_r.at[q, k], updev if d == 0 else dndev)

    def ag_side(q, which, k):
        ref = held(q, c, which, k)
        return rdma(ref, ref, sent.at[1], ags_r.at[q, k], xdev if k < quar else ydev)

    def ag_part(q, which, k):
        ref = held(q, c, which, k)
        return rdma(ref, ref, sent.at[2], agp_r, partner)

    def own_part():
        ref = whole.at[pl.ds(s * cap, cap)]
        return rdma(ref, ref, sent.at[2], agp_r, partner)

    def slots_of(count, ss, rs):
        ref = whole.at[pl.ds(0, count)]
        return rdma(ref, ref, ss, rs, partner)

    def onward(zz, q):
        out = []
        if q <= zz < planes - 1:
            out.append(0)
        if q >= zz > 0:
            out.append(1)
        return out

    def d_copy(j, i):
        blocks = pl.ds(i * nb, nb)
        return rdma(
            part.at[oc, j, :, blocks], drecv.at[j, :, blocks], sent.at[3], d_r.at[j, i], partner
        )

    def first_hop(j, i, n):
        q, dev = (xq, xdev) if j % 2 == 0 else (yq, ydev)
        q = (q, dq)[n]
        blocks = pl.ds(i * nb, nb)
        return rdma(
            part.at[c, j, q, blocks], r1.at[j, n, blocks], sent.at[4], r1_r.at[j, i, n], dev
        )

    def second_hop(j, i):
        far, dev = (yq, ydev) if j % 2 == 0 else (xq, xdev)
        blocks = pl.ds(i * nb, nb)
        return rdma(
            part.at[c, j, far, blocks], r2.at[j, blocks], sent.at[5], r2_r.at[j], dev
        )

    def add_to(dst, src, start, count):
        step = next(n for n in (10, 8, 5, 4, 2, 1) if count % n == 0)

        def body(i, carry):
            sl = pl.ds(start + i * step, step)
            dst[sl] = (dst[sl].astype(F32) + src[sl].astype(F32)).astype(BF16)
            return carry

        lax.fori_loop(0, count // step, body, 0)

    def second_got(j):
        ref = r2.at[j]
        return rdma(ref, ref, sent.at[5], r2_r.at[j], partner)

    def z_copy(j, q, up, here):
        if up:
            return rdma(slots.at[j, q], zup.at[j, q], sent.at[6], z_r.at[j, q], updev)
        k = planes if q == here else q
        return rdma(slots.at[j, q], zdn.at[j, q], sent.at[7], z_r.at[j, k], dndev)

    my_id = quad * 2 + c

    def f_copies(zz, j):
        out = []
        for n, dev in enumerate(near):
            cc = oc if n in (0, 2, 4) else c
            onward_there = n in ((1, 2) if j % 2 == 0 else (3, 4))
            out.append(
                rdma(
                    slots.at[j, zz, pl.ds(cc * cap, cap)], frecv.at[j, my_id],
                    sent.at[8], pass_r.at[j] if onward_there else end_r, dev,
                )
            )
        return out

    def f_pass(j):
        q, dev = (xq, ydev) if j % 2 == 0 else (yq, xdev)
        pair = frecv.at[j, pl.ds(q * 2, 2)]
        return rdma(pair, pair, sent.at[8], end_r, dev)

    def f_pair(j):
        pair = frecv.at[j, pl.ds(0, 2)]
        return rdma(pair, pair, sent.at[8], pass_r.at[j], partner)

    def f_all(ss, rs, count):
        ref = frecv.at[:, pl.ds(0, count)]
        return rdma(ref, ref, ss, rs, partner)

    def g_copy(n):
        dev = (partner, xdev, ydev, ddev)[n]
        return rdma(gst.at[min(n, 1)], grecv.at[n], sent.at[9], g_r.at[n], dev)

    def gz_copy(d, q):
        return rdma(gst.at[2], gz.at[q], sent.at[9], gz_r, others[d - 1])

    def g_all(ref, ss, rs):
        return rdma(ref, ref, ss, rs, partner)

    def squares(i, acc):
        v = tok[:, pl.ds(pl.multiple_of(i * 2 * BLK, 2 * BLK), 2 * BLK)].astype(F32)
        v = v * v
        return acc + v[:, :BLK] + v[:, BLK:]

    def term(i, carry):
        cols = pl.ds(pl.multiple_of(i * wide, wide), wide)
        normed = (tok[:, cols].astype(F32) * inv[...] * gain[:, cols]).astype(BF16)
        res = lax.dot_general(
            normed, cot[...], (((0,), (0,)), ((), ())), preferred_element_type=F32
        )
        res = (res * scale).astype(BF16)
        group = res.shape[1] // (2 * QUAD)
        tgrad[:, cols] = normed
        for b in range(wide // BLK):
            for j in range(NJ):
                lo = b * BLK + j * SUB
                for k in range(QUAD):
                    for cc in range(2):
                        col = (k * 2 + cc) * group
                        part[cc, j, k, i * (wide // BLK) + b] = res[lo:lo + SUB, col:col + group]
        return carry

    def weight_group(g, grp):
        return jnp.concatenate([whole[slot_of[g * grp + i]] for i in range(grp)], axis=0)

    def cuts(grp, a):
        groups = nblk // grp
        return groups * a // COMPUTE, groups * (a + 1) // COMPUTE

    def fwd_body(g, carry):
        gw = FGRP * BLK
        cols = pl.ds(pl.multiple_of(g * gw, gw), gw)
        fwd[...] += jnp.dot(tgrad[:, cols], weight_group(g, FGRP), preferred_element_type=F32)
        return carry

    def bwd_body(g, carry):
        gw = BGRP * BLK
        cols = pl.ds(pl.multiple_of(g * gw, gw), gw)
        grad = lax.dot_general(
            cot[...], weight_group(g, BGRP), (((1,), (1,)), ((), ())), preferred_element_type=F32
        )
        values = tok[:, cols].astype(F32)
        grad = grad * inv[...]
        tgrad[:, cols] = (grad * gain[:, cols] - values * coef[...]).astype(BF16)
        gst[0, :, cols] = jnp.sum(grad * values, axis=0, keepdims=True) * scale
        return carry

    def shared_step(step, a):
        if step == SQ:
            loads[1].wait()
            acc = lax.fori_loop(
                0, width // (2 * BLK), squares, jnp.zeros((tokens_here, BLK), F32)
            )
            inv[...] = lax.rsqrt(jnp.sum(acc, axis=1, keepdims=True) / width + EPS)
            for cp in loads[2:]:
                cp.wait()
        elif step == TERM:
            count = width // wide
            lax.fori_loop(a * count // NI, (a + 1) * count // NI, term, 0)
            for j in range(NJ):
                d_copy(j, a).start()
        elif step == FWD:
            if a == 0:
                fwd[...] = jnp.zeros_like(fwd)
            lax.fori_loop(*cuts(FGRP, a), fwd_body, 0)
        else:
            if a == 0:
                total = fwd[...]
                proj[...] = (total + bias[...]).astype(BF16)
                inner = jnp.sum(total * cot[...].astype(F32), axis=1, keepdims=True) / width
                coef[...] = inv[...] * inv[...] * inner
                gst[0, :, width:] = jnp.sum(cot[...].astype(F32), axis=0, keepdims=True) * scale
            lax.fori_loop(*cuts(BGRP, a), bwd_body, 0)

    def own_step(zz, step, a, b):
        if step == OWN:
            for d in onward(zz, zz):
                ag_z(zz, d, a).start()
        elif step == OWNP:
            own_part().start()
        elif step == OWNER:
            lax.fori_loop(0, 2 * planes * cap, owner, 0)
        elif step == AGZ:
            ag_z(a, 0, b).wait_recv()
            for d in onward(zz, a):
                ag_z(a, d, b).start()
            ag_part(a, 0, b).start()
        elif step == AGSIDE:
            ag_side(a, 0, b).start()
        elif step == AGPART:
            ag_side(a, 1, b).wait_recv()
            ag_part(a, 1, b).start()
        elif step == AGEND:
            slots_of(planes * cap, sent.at[2], agp_r).wait_recv()
        elif step == SUM:
            d_copy(a, b).wait_recv()
            for k in range(QUAD):
                add_to(part.at[c, a, k], drecv.at[a, k], b * nb, nb)
        elif step == HOP1:
            first_hop(a, b, 1).start()
            first_hop(a, b, 0).start()
        elif step == HOP2:
            far = yq if a % 2 == 0 else xq
            first_hop(a, b, 1).wait_recv()
            add_to(part.at[c, a, far], r1.at[a, 1], b * nb, nb)
            second_hop(a, b).start()
            first_hop(a, b, 0).wait_recv()
            add_to(part.at[c, a, quad], r1.at[a, 0], b * nb, nb)
        elif step == PLACE:
            second_got(a).wait_recv()
            add_to(part.at[c, a, quad], r2.at[a], 0, nblk)

            def body(i, carry):
                for u in range(per_plane):
                    k = bos[i * per_plane + u]
                    val = part[c, a, quad, jnp.maximum(k, 0)]
                    slots[a, i, u] = jnp.where(k >= 0, val.astype(F32), 0.0).astype(BF16)
                return carry

            lax.fori_loop(0, planes, body, 0)
        elif step == ZUP:
            if zz > 0:
                z_copy(a, b, True, zz).wait_recv()
                add_to(slots.at[a, b], zup.at[a, b], 0, per_plane)
            z_copy(a, b, True, zz).start()
        elif step == ZDN:
            if zz < planes - 1:
                z_copy(a, b, False, zz).wait_recv()
                add_to(slots.at[a, b], zdn.at[a, b], 0, per_plane)
            z_copy(a, b, False, zz - 1).start()
        elif step == ZEND:
            if zz > 0:
                z_copy(a, zz, True, zz).wait_recv()
                add_to(slots.at[a, zz], zup.at[a, zz], 0, per_plane)
            if zz < planes - 1:
                z_copy(a, zz, False, zz).wait_recv()
                add_to(slots.at[a, zz], zdn.at[a, zz], 0, per_plane)
            for cp in f_copies(zz, a):
                cp.start()
            frecv[a, my_id] = slots[a, zz, pl.ds(c * cap, cap)]
        elif step == PASS:
            f_pair(a).wait_recv()
            f_pass(a).start()
        elif step == G0:
            g_copy(0).start()
        elif step == GSTEP:
            if a == 0:
                g_copy(0).wait_recv()
                gst[1] = gst[0] + grecv[0]
                for n in (3, 1, 2):
                    g_copy(n).start()
            else:
                for n in (1, 2, 3):
                    g_copy(n).wait_recv()
                gst[2] = (gst[1] + grecv[1]) + (grecv[2] + grecv[3])
                gz[zz] = gst[2]
                for d in range(1, planes):
                    gz_copy(d, zz).start()
        elif step == GEND:
            g_all(gz.at[pl.ds(0, planes - 1)], sent.at[9], gz_r).wait_recv()
            total = gz[0]
            for q in range(1, planes):
                total = total + gz[q]
            vec[...] = total

    def finish(zz):
        f_all(sent.at[8], end_r, 5).wait_recv()
        count = sum(len(onward(zz, q)) for q in range(planes)) * half
        slots_of(count, sent.at[0], agp_r).wait_send()
        slots_of((planes - 1) * half, sent.at[1], agp_r).wait_send()
        slots_of(planes * cap, sent.at[2], agp_r).wait_send()
        rdma(drecv, drecv, sent.at[3], end_r, partner).wait_send()
        rdma(r1, r1, sent.at[4], end_r, partner).wait_send()
        rdma(r2, r2, sent.at[5], end_r, partner).wait_send()
        for n, count in ((6, planes - 1 - zz), (7, zz)):
            if count:
                ref = slots.at[:, pl.ds(0, count)]
                rdma(ref, ref, sent.at[n], end_r, partner).wait_send()
        f_all(sent.at[8], end_r, 7).wait_send()
        g_all(gz.at[pl.ds(0, planes - 1)], sent.at[9], gz_r).wait_send()
        g_all(grecv, sent.at[9], gz_r).wait_send()

    plans = [split(order_of(zz, planes, cap)) for zz in range(planes)]
    common = plans[0][1]
    for n in range(len(common) + 1):
        for zz in range(planes):
            assert plans[zz][1] == common
            todo = plans[zz][0][n]
            last = n == len(common)
            if todo or last:
                @pl.when(z == zz)
                def _():
                    for tk in todo:
                        own_step(zz, *tk)
                    if last:
                        finish(zz)

        if n < len(common):
            shared_step(*common[n][:2])


def write_kernel(proj, tgrad, frecv, vec, proj_h, tgrad_h, wgrad_h, gain_h, bias_h, buf, sem, wsem):
    width = gain_h.shape[1]
    cap = frecv.shape[2]
    copies = [
        pltpu.make_async_copy(tgrad, tgrad_h, sem.at[0]),
        pltpu.make_async_copy(proj, proj_h, sem.at[1]),
        pltpu.make_async_copy(vec.at[:, :width], gain_h, sem.at[2]),
        pltpu.make_async_copy(vec.at[:, width:], bias_h, sem.at[3]),
    ]
    for cp in copies:
        cp.start()
    for u in range(cap):
        for j in range(NJ):
            for n in range(2 * QUAD):
                buf[u, j * SUB:(j + 1) * SUB, n * BLK:(n + 1) * BLK] = frecv[j, n, u].astype(F32)
        cp = pltpu.make_async_copy(buf.at[u], wgrad_h.at[u], wsem.at[u])
        cp.start()
        copies.append(cp)
    for cp in copies:
        cp.wait()


def communicate(tokens, norm_gain, cotangent, key_bias, block_slot, key_weight, scale):
    shard_count = lax.axis_size("shard")
    planes = shard_count // 2
    rows, cols = key_weight.shape
    cap = rows // BLK
    half = cap // 2
    tok_count, width = tokens.shape
    nblk = width // BLK
    group = cols // (2 * QUAD)
    dma = pltpu.SemaphoreType.DMA
    vm = pltpu.VMEM
    hbm = pl.BlockSpec(memory_space=pl.ANY)
    local = pl.BlockSpec(memory_space=vm)
    held = pl.pallas_call(
        functools.partial(comm_kernel, planes, cap, nblk, scale),
        out_shape=(
            vm((tok_count, cols), BF16),
            vm((tok_count, width), BF16),
            vm((NJ, 2 * QUAD, cap, SUB, group), BF16),
            vm((1, width + cols), F32),
        ),
        in_specs=[hbm, hbm, hbm, hbm, hbm, pl.BlockSpec(memory_space=pltpu.SMEM)],
        out_specs=(local,) * 4,
        scratch_shapes=[
            vm((shard_count * cap, BLK, cols), BF16),
            vm((tok_count, width), BF16),
            vm((tok_count, cols), BF16),
            vm((1, width), F32),
            vm((1, cols), F32),
            vm((tok_count, 1), F32),
            vm((tok_count, 1), F32),
            vm((tok_count, cols), F32),
            vm((3, 1, width + cols), F32),
            vm((4, 1, width + cols), F32),
            vm((planes, 1, width + cols), F32),
            vm((2, NJ, QUAD, nblk, SUB, group), BF16),
            vm((NJ, QUAD, nblk, SUB, group), BF16),
            vm((NJ, 2, nblk, SUB, group), BF16),
            vm((NJ, nblk, SUB, group), BF16),
            vm((NJ, planes, 2 * cap, SUB, group), BF16),
            vm((NJ, planes, 2 * cap, SUB, group), BF16),
            vm((NJ, planes, 2 * cap, SUB, group), BF16),
            pltpu.SMEM((shard_count * cap,), jnp.int32),
            dma((5,)),
            dma((planes, half)), dma((planes, half)), dma(()),
            dma((NJ, NI)), dma((NJ, NI, 2)), dma((NJ,)), dma((NJ, planes + 1)),
            dma((NJ,)), dma(()), dma((4,)), dma(()), dma((10,)),
        ],
        compiler_params=pltpu.CompilerParams(
            collective_id=0, has_side_effects=True, vmem_limit_bytes=54 * 2**20
        ),
    )(
        tokens, norm_gain[None, :], cotangent, key_bias[None, :],
        key_weight.reshape(cap, BLK, cols), block_slot,
    )
    return pl.pallas_call(
        write_kernel,
        out_shape=(
            jax.ShapeDtypeStruct((tok_count, cols), BF16),
            jax.ShapeDtypeStruct((tok_count, width), BF16),
            jax.ShapeDtypeStruct((cap, BLK, cols), F32),
            jax.ShapeDtypeStruct((1, width), F32),
            jax.ShapeDtypeStruct((1, cols), F32),
        ),
        in_specs=[local] * 4,
        out_specs=(hbm,) * 5,
        scratch_shapes=[vm((cap, BLK, cols), F32), dma((4,)), dma((cap,))],
        compiler_params=pltpu.CompilerParams(vmem_limit_bytes=8 * 2**20),
    )(*held)


def local(tokens, norm_gain, key_bias, key_weight, cotangent, block_slot):
    row_count, width = tokens.shape
    shard_count = lax.axis_size("shard")
    replicas = lax.axis_size("rep")
    grad_scale = float(row_count * shard_count * replicas) ** (-0.5)
    projected, token_grad, weight_grad, gain_grad, bias_grad = communicate(
        tokens, norm_gain, cotangent, key_bias, block_slot, key_weight, grad_scale
    )
    weight_grad = weight_grad.reshape(key_weight.shape)
    if replicas > QUAD:
        groups = [list(range(i, replicas, QUAD)) for i in range(QUAD)]
        weight_grad, gain_grad, bias_grad = lax.psum(
            (weight_grad, gain_grad, bias_grad), "rep", axis_index_groups=groups
        )
    return (projected, token_grad, weight_grad, gain_grad[0], bias_grad[0])


def solution(mesh):
    return jax.shard_map(
        local,
        mesh=mesh,
        in_specs=(
            P(("shard", "rep"), None),
            P(),
            P(),
            P("shard", None),
            P(("shard", "rep"), None),
            P(),
        ),
        out_specs=(
            P(("shard", "rep"), None),
            P(("shard", "rep"), None),
            P("shard", None),
            P(),
            P(),
        ),
        check_vma=False,
    )
```

```python
import functools
import jax
import jax.numpy as jnp
from jax import lax
from jax.experimental import pallas as pl
from jax.experimental.pallas import tpu as pltpu
from jax.sharding import PartitionSpec as P

BLK = 128
EPS = 1e-06
NJ = 8
NI = 4
SUB = BLK // NJ
HROW = BLK // 2
QUAD = 4
MESH = pl.DeviceIdType.MESH
F32 = jnp.float32
BF16 = jnp.bfloat16
COMPUTE = 3
BGRP = 8

OWN, OWNP, SQ, TERM, SUM, HOP1, HOP2, PLACE, ZUP, ZDN, ZEND, PASS = range(12)
FWD, BWD, AGZ, AGSIDE, AGPART, G0, GSTEP, GEND, OWNER, RAW, OWNX = range(12, 23)
COMMON = (SQ, TERM, FWD, BWD)

TUNED = (
    (
        (OWN, 0, 0), (OWN, 1, 0), (OWN, 2, 0), (OWN, 3, 0), (OWN, 4, 0), (OWN, 5, 0), (OWN, 6, 0),
        (OWN, 7, 0), (OWNP, 0, 0), (SQ, 0, 0), (TERM, 0, 0), (TERM, 1, 0), (SUM, 1, 0), (HOP1, 1, 0),
        (SUM, 4, 0), (AGZ, 1, 0), (AGSIDE, 1, 0), (SUM, 3, 0), (TERM, 2, 0), (SUM, 2, 0), (SUM, 0, 0),
        (SUM, 1, 1), (HOP1, 4, 0), (HOP1, 1, 1), (HOP1, 2, 0), (OWNX, 0, 7), (HOP1, 3, 0), (SUM, 5, 1),
        (SUM, 6, 0), (SUM, 3, 1), (TERM, 3, 0), (HOP1, 5, 1), (SUM, 2, 1), (SUM, 6, 2), (SUM, 0, 2),
        (SUM, 7, 0), (SUM, 4, 1), (SUM, 4, 2), (SUM, 3, 2), (SUM, 0, 3), (HOP1, 0, 0), (AGZ, 1, 2),
        (SUM, 2, 3), (SUM, 3, 3), (HOP1, 0, 2), (SUM, 0, 1), (SUM, 5, 2), (AGZ, 1, 3), (HOP1, 2, 1),
        (SUM, 1, 3), (HOP2, 1, 0), (SUM, 5, 0), (SUM, 1, 2), (HOP1, 3, 2), (HOP1, 3, 3), (SUM, 7, 3),
        (HOP2, 0, 0), (HOP1, 4, 2), (SUM, 4, 3), (AGZ, 1, 4), (HOP1, 1, 3), (HOP1, 2, 3), (HOP1, 4, 3),
        (AGSIDE, 1, 4), (HOP1, 0, 1), (SUM, 6, 1), (RAW, 7, 0), (OWNX, 0, 3), (HOP2, 2, 1), (SUM, 5, 3),
        (HOP1, 5, 3), (AGZ, 1, 6), (AGZ, 1, 1), (HOP2, 2, 0), (AGSIDE, 1, 2), (AGZ, 1, 5), (HOP1, 4, 1),
        (HOP1, 0, 3), (AGSIDE, 1, 6), (SUM, 6, 3), (RAW, 6, 0), (HOP2, 3, 0), (RAW, 6, 1), (SUM, 7, 1),
        (HOP1, 1, 2), (AGPART, 1, 2), (HOP2, 5, 1), (SUM, 2, 2), (HOP1, 3, 1), (SUM, 7, 2), (HOP2, 5, 3),
        (AGZ, 2, 6), (HOP2, 4, 0), (HOP2, 1, 1), (HOP2, 0, 2), (AGZ, 2, 1), (HOP2, 1, 3), (HOP2, 1, 2),
        (AGSIDE, 1, 3), (RAW, 7, 2), (HOP2, 4, 1), (AGSIDE, 2, 6), (HOP2, 0, 3), (HOP2, 3, 1), (HOP2, 4, 3),
        (AGSIDE, 1, 1), (HOP2, 4, 2), (OWNER, 0, 0), (HOP2, 3, 2), (AGZ, 1, 7), (AGPART, 1, 0), (HOP2, 2, 3),
        (RAW, 6, 3), (RAW, 6, 2), (HOP2, 0, 1), (HOP1, 2, 2), (HOP1, 5, 0), (AGZ, 2, 5), (PLACE, 1, 0),
        (ZUP, 1, 2), (HOP1, 5, 2), (AGSIDE, 2, 1), (FWD, 0, 0), (PLACE, 0, 0), (PLACE, 4, 0), (ZUP, 4, 3),
        (AGSIDE, 1, 5), (HOP2, 3, 3), (AGPART, 1, 3), (AGZ, 2, 4), (HOP2, 5, 2), (AGZ, 2, 3), (ZUP, 0, 3),
        (HOP2, 2, 2), (AGZ, 3, 2), (AGZ, 2, 0), (AGZ, 2, 2), (AGPART, 1, 4), (RAW, 7, 3), (AGSIDE, 1, 7),
        (AGSIDE, 2, 3), (PLACE, 3, 0), (AGZ, 2, 7), (AGSIDE, 2, 5), (AGSIDE, 2, 7), (HOP2, 5, 0), (AGSIDE, 3, 2),
        (AGSIDE, 2, 0), (AGPART, 2, 6), (AGPART, 1, 7), (AGZ, 3, 7), (ZUP, 1, 3), (AGSIDE, 3, 7), (PLACE, 5, 0),
        (ZUP, 3, 3), (RAW, 7, 1), (PLACE, 2, 0), (AGPART, 2, 1), (AGPART, 1, 5), (AGPART, 2, 7), (AGSIDE, 2, 2),
        (AGZ, 3, 0), (AGZ, 3, 5), (ZUP, 5, 3), (ZUP, 0, 1), (AGSIDE, 3, 5), (AGZ, 3, 1), (AGSIDE, 3, 0),
        (AGPART, 3, 7), (AGSIDE, 2, 4), (AGSIDE, 3, 1), (ZUP, 0, 2), (AGZ, 3, 3), (AGPART, 2, 5), (ZUP, 1, 1),
        (ZUP, 2, 3), (AGPART, 2, 2), (AGPART, 1, 1), (AGPART, 3, 2), (ZUP, 2, 2), (AGSIDE, 3, 3), (AGPART, 1, 6),
        (ZUP, 3, 2), (AGZ, 3, 6), (AGSIDE, 3, 6), (AGZ, 3, 4), (AGSIDE, 3, 4), (AGPART, 2, 0), (AGPART, 3, 5),
        (AGPART, 2, 3), (AGPART, 2, 4), (ZUP, 4, 2), (FWD, 1, 0), (AGPART, 3, 1), (ZUP, 2, 1), (ZUP, 5, 2),
        (ZEND, 1, 0), (FWD, 2, 0), (AGPART, 3, 6), (AGPART, 3, 3), (AGPART, 3, 0), (ZEND, 4, 0), (ZUP, 3, 1),
        (AGPART, 3, 4), (ZEND, 0, 0), (ZUP, 5, 1), (ZEND, 3, 0), (ZUP, 4, 1), (FWD, 3, 0), (PASS, 4, 0),
        (ZEND, 5, 0), (BWD, 0, 0), (PASS, 0, 0), (PASS, 1, 0), (PASS, 3, 0), (BWD, 1, 0), (ZEND, 2, 0),
        (BWD, 2, 0), (G0, 0, 0), (GSTEP, 0, 0), (ZEND, 6, 0), (PASS, 5, 0), (ZEND, 7, 0), (PASS, 2, 0),
        (GSTEP, 1, 0), (PASS, 7, 0), (PASS, 6, 0), (GEND, 0, 0),
    ),
    (
        (OWN, 0, 0), (OWN, 1, 0), (OWN, 2, 0), (OWN, 3, 0), (OWN, 4, 0), (OWN, 5, 0), (OWN, 6, 0),
        (OWN, 7, 0), (OWNP, 0, 0), (SQ, 0, 0), (TERM, 0, 0), (TERM, 1, 0), (SUM, 0, 0), (SUM, 1, 0),
        (HOP1, 0, 0), (HOP1, 1, 0), (SUM, 3, 0), (AGZ, 0, 0), (TERM, 2, 0), (SUM, 5, 0), (HOP1, 5, 0),
        (SUM, 4, 0), (SUM, 3, 1), (AGSIDE, 0, 0), (SUM, 5, 1), (SUM, 2, 0), (HOP1, 3, 0), (SUM, 5, 2),
        (SUM, 0, 1), (SUM, 1, 1), (HOP1, 1, 1), (HOP2, 1, 0), (HOP1, 2, 0), (HOP1, 0, 1), (SUM, 2, 1),
        (AGZ, 0, 2), (SUM, 1, 2), (HOP2, 0, 0), (AGSIDE, 0, 2), (AGZ, 0, 1), (HOP1, 3, 1), (SUM, 2, 2),
        (OWNX, 0, 6), (TERM, 3, 0), (HOP1, 5, 1), (HOP2, 2, 0), (HOP1, 4, 0), (SUM, 4, 2), (SUM, 4, 3),
        (SUM, 0, 3), (HOP1, 1, 2), (OWNER, 0, 0), (HOP1, 5, 2), (SUM, 3, 2), (HOP1, 0, 3), (HOP1, 3, 2),
        (AGZ, 2, 1), (HOP1, 4, 2), (HOP1, 4, 3), (AGZ, 2, 6), (AGZ, 0, 3), (HOP2, 3, 0), (SUM, 5, 3),
        (AGZ, 2, 3), (SUM, 2, 3), (HOP2, 5, 0), (SUM, 4, 1), (HOP1, 5, 3), (AGZ, 0, 4), (AGSIDE, 0, 1),
        (AGZ, 0, 5), (FWD, 1, 0), (AGZ, 2, 0), (OWNX, 0, 3), (HOP1, 4, 1), (HOP1, 2, 3), (AGZ, 0, 7),
        (SUM, 1, 3), (HOP2, 5, 2), (HOP2, 5, 1), (HOP1, 1, 3), (AGZ, 2, 2), (AGZ, 0, 6), (AGSIDE, 0, 5),
        (HOP2, 3, 2), (HOP1, 2, 2), (AGSIDE, 0, 4), (SUM, 7, 0), (HOP2, 5, 3), (AGZ, 2, 5), (AGPART, 0, 0),
        (AGZ, 3, 2), (AGZ, 2, 4), (AGZ, 2, 7), (AGSIDE, 2, 5), (AGSIDE, 0, 6), (SUM, 3, 3), (AGPART, 2, 6),
        (HOP2, 1, 2), (HOP2, 0, 3), (SUM, 6, 0), (HOP2, 2, 3), (HOP2, 4, 0), (AGPART, 0, 4), (HOP1, 3, 3),
        (SUM, 0, 2), (OWNX, 0, 7), (AGSIDE, 2, 4), (AGSIDE, 2, 0), (HOP1, 2, 1), (SUM, 6, 1), (HOP2, 4, 2),
        (HOP1, 0, 2), (PLACE, 5, 0), (SUM, 7, 2), (AGZ, 3, 5), (HOP2, 4, 1), (AGSIDE, 2, 1), (HOP2, 4, 3),
        (HOP2, 0, 1), (AGPART, 0, 7), (AGSIDE, 3, 5), (AGPART, 0, 6), (OWNX, 0, 2), (HOP1, 6, 0), (HOP1, 7, 0),
        (AGPART, 0, 1), (SUM, 6, 3), (AGZ, 3, 7), (HOP2, 1, 1), (HOP2, 0, 2), (HOP2, 1, 3), (HOP2, 2, 1),
        (AGPART, 2, 0), (HOP2, 3, 3), (SUM, 6, 2), (AGZ, 3, 0), (AGSIDE, 3, 7), (AGZ, 3, 1), (PLACE, 4, 0),
        (AGZ, 3, 6), (HOP1, 6, 2), (AGSIDE, 3, 6), (HOP2, 3, 1), (HOP1, 6, 1), (HOP2, 2, 2), (AGPART, 2, 3),
        (AGZ, 3, 3), (AGPART, 2, 4), (AGPART, 0, 5), (ZUP, 4, 3), (PLACE, 0, 0), (ZUP, 0, 3), (AGSIDE, 3, 2),
        (AGPART, 3, 5), (AGPART, 2, 2), (HOP1, 6, 3), (HOP2, 6, 1), (PLACE, 1, 0), (AGPART, 0, 2), (AGPART, 2, 7),
        (AGZ, 3, 4), (AGPART, 2, 5), (ZUP, 1, 3), (HOP2, 6, 2), (PLACE, 3, 0), (AGSIDE, 3, 0), (AGPART, 2, 1),
        (AGPART, 0, 3), (ZDN, 1, 0), (ZUP, 1, 2), (AGSIDE, 3, 4), (AGPART, 3, 7), (HOP2, 6, 0), (PLACE, 2, 0),
        (AGSIDE, 3, 1), (FWD, 2, 0), (AGPART, 3, 0), (HOP1, 7, 2), (AGSIDE, 3, 3), (SUM, 7, 3), (ZDN, 0, 0),
        (ZUP, 3, 3), (FWD, 0, 0), (ZDN, 4, 0), (ZUP, 5, 3), (HOP2, 6, 3), (AGPART, 3, 1), (ZUP, 0, 2),
        (HOP1, 7, 3), (ZDN, 3, 0), (AGPART, 3, 2), (AGPART, 3, 6), (AGPART, 3, 4), (HOP2, 7, 0), (HOP2, 7, 2),
        (SUM, 7, 1), (HOP1, 7, 1), (ZUP, 2, 3), (AGPART, 3, 3), (PLACE, 6, 0), (ZEND, 1, 0), (ZDN, 5, 0),
        (ZUP, 2, 2), (ZEND, 0, 0), (ZUP, 6, 2), (FWD, 3, 0), (ZUP, 3, 2), (HOP2, 7, 3), (HOP2, 7, 1),
        (ZUP, 6, 3), (BWD, 0, 0), (ZEND, 2, 0), (ZDN, 2, 0), (ZUP, 4, 2), (ZEND, 6, 0), (BWD, 1, 0),
        (PASS, 0, 0), (PLACE, 7, 0), (ZEND, 3, 0), (PASS, 1, 0), (ZDN, 6, 0), (ZUP, 7, 3), (ZUP, 7, 2),
        (BWD, 2, 0), (G0, 0, 0), (ZEND, 4, 0), (ZUP, 5, 2), (ZDN, 7, 0), (GSTEP, 0, 0), (ZEND, 7, 0),
        (ZEND, 5, 0), (PASS, 6, 0), (GSTEP, 1, 0), (PASS, 3, 0), (PASS, 4, 0), (PASS, 7, 0), (PASS, 2, 0),
        (PASS, 5, 0), (GEND, 0, 0),
    ),
)


MOVED = (6, 7)
DIRECT = {(0, 1): (), (1, 0): (7, 3), (1, 2): (7, 3, 6, 2)}


def moved_of(planes, cap):
    return MOVED if planes == 4 and cap == 8 else ()


def direct_of(to, of, planes, cap):
    if planes != 4 or cap != 8:
        return ()
    if 2 * to >= planes:
        to, of = planes - 1 - to, planes - 1 - of
    return DIRECT.get((to, of), ())


def mirror(order, planes):
    flip = {ZUP: ZDN, ZDN: ZUP}
    out = []
    for step, a, b in order:
        if step in (ZUP, ZDN):
            b = planes - 1 - b
        if step in (AGZ, AGSIDE, AGPART, FWD):
            a = planes - 1 - a
        if step == OWNX:
            a = 1 - a
        out.append((flip.get(step, step), a, b))
    return out


def plain_order(z, planes, cap):
    half = cap
    out = [(OWN, k, 0) for k in range(half)] + [(OWNP, 0, 0), (SQ, 0, 0), (OWNER, 0, 0)]
    out += [(TERM, i, 0) for i in range(NI)]
    for step in (SUM, HOP1, HOP2):
        out += [(step, j, i) for j in range(NJ) for i in range(NI)]
    out += [(PLACE, j, 0) for j in range(NJ)]
    for step in (AGZ, AGSIDE, AGPART):
        for t in range(1, planes):
            for q in (z - t, z + t):
                if 0 <= q < planes:
                    out += [(step, q, k) for k in range(half)]
    for t in range(planes - 1):
        for j in range(NJ):
            if z < planes - 1 - t:
                out.append((ZUP, j, planes - 1 - t))
            if z > t:
                out.append((ZDN, j, t))
    for step in (ZEND, PASS):
        out += [(step, j, 0) for j in range(NJ)]
    out += [(FWD, q, 0) for q in range(planes)]
    out += [(BWD, g, 0) for g in range(COMPUTE)]
    out.append((G0, 0, 0))
    out += [(GSTEP, n, 0) for n in range(2)]
    out.append((GEND, 0, 0))
    return out


def order_of(z, planes, cap):
    if planes == 4 and cap == 8:
        return list(TUNED[z]) if z < 2 else mirror(TUNED[planes - 1 - z], planes)
    return plain_order(z, planes, cap)


def split(order):
    parts, common, gathered = [[]], [], []
    for tok in order:
        if tok[0] in COMMON:
            if tok[0] == FWD:
                gathered.append(tok[1])
                tok = (FWD, len(gathered) - 1, 0)
            common.append(tok)
            parts.append([])
        else:
            parts[-1].append(tok)
    return parts, common, gathered


def comm_kernel(
    planes, cap, nblk, scale,
    tok_h, gain_h, cot_h, bias_h, w_h, slot_of,
    proj, tgrad, frecv, vec,
    whole, tok, cot, gain, bias, inv, coef, fwd, gst, grecv, gz,
    part, drecv, r1, r2, raw, slots, zup, zdn, bos,
    in_sem, agz_r, ags_r, agp_r, d_r, r1_r, r2_r, raw_r, z_r, pass_r, end_r, g_r, gz_r, sent,
):
    s = lax.axis_index("shard")
    r = lax.axis_index("rep")
    z = s // 2
    c = s % 2
    quad = r % QUAD
    base = r - quad
    y = quad // 2
    x = quad % 2
    xq = y * 2 + (1 - x)
    yq = (1 - y) * 2 + x
    dq = (1 - y) * 2 + (1 - x)
    oc = 1 - c
    partner = (2 * z + oc, r)
    xdev = (s, base + xq)
    ydev = (s, base + yq)
    updev = (s + 2, r)
    dndev = (s - 2, r)
    ddev = (s, base + dq)
    near = [partner] + [(2 * z + cc, base + q) for q in (xq, yq) for cc in (c, oc)]
    others = [(2 * ((z + d) % planes) + c, r) for d in range(1, planes)]

    bar = pltpu.get_barrier_semaphore()
    greet = near + [ddev] + others
    for dev in greet:
        pl.semaphore_signal(bar, inc=1, device_id=dev, device_id_type=MESH)

    loads = [
        pltpu.make_async_copy(w_h, whole.at[pl.ds(s * cap, cap)], in_sem.at[0]),
        pltpu.make_async_copy(tok_h, tok, in_sem.at[1]),
        pltpu.make_async_copy(cot_h, cot, in_sem.at[2]),
        pltpu.make_async_copy(gain_h, gain, in_sem.at[3]),
        pltpu.make_async_copy(bias_h, bias, in_sem.at[4]),
    ]
    for cp in loads:
        cp.start()

    def owner(u, carry):
        found = jnp.int32(-1)
        for b in range(nblk):
            found = jnp.where(slot_of[b] == u, b, found)
        bos[u] = found
        return carry

    loads[0].wait()
    pl.semaphore_wait(bar, len(greet))

    def rdma(src, dst, ss, rs, dev):
        return pltpu.make_async_remote_copy(
            src_ref=src, dst_ref=dst, send_sem=ss, recv_sem=rs, device_id=dev, device_id_type=MESH
        )

    moved = moved_of(planes, cap)
    half = cap
    quar = cap // 2
    hh = (x + y) % 2
    tokens_here, width = tok.shape
    wide = 5 * BLK
    nb = nblk // NI
    per_plane = 2 * cap

    def held(q, core, which, k):
        start = (hh if which == 0 else 1 - hh) * (cap // 2) + k // 2
        return whole.at[pl.ds((2 * q + core) * cap + start, 1), pl.ds(k % 2 * HROW, HROW)]

    def ag_z(q, d, k):
        ref = held(q, c, 0, k)
        return rdma(ref, ref, sent.at[0], agz_r.at[q, k], updev if d == 0 else dndev)

    def ag_side(q, which, k):
        ref = held(q, c, which, k)
        return rdma(ref, ref, sent.at[1], ags_r.at[q, k], xdev if k < quar else ydev)

    def ag_direct(zz, d, k):
        ref = held(zz, c, 1, k)
        return rdma(ref, ref, sent.at[0], ags_r.at[zz, k], updev if d == 0 else dndev)

    def direct(to, of):
        return direct_of(to, of, planes, cap) if 0 <= to < planes and 0 <= of < planes else ()

    def ag_part(q, which, k):
        ref = held(q, c, which, k)
        return rdma(ref, ref, sent.at[2], agp_r.at[q], partner)

    def own_part():
        ref = whole.at[pl.ds(s * cap, cap)]
        return rdma(ref, ref, sent.at[2], agp_r.at[z], partner)

    def chunks_of(count, ss, rs):
        ref = whole.at[pl.ds(0, count), pl.ds(0, HROW)]
        return rdma(ref, ref, ss, rs, partner)

    def onward(zz, q):
        out = []
        if q <= zz < planes - 1:
            out.append(0)
        if q >= zz > 0:
            out.append(1)
        return out

    def d_copy(j, i):
        blocks = pl.ds(i * nb, nb)
        return rdma(
            part.at[oc, j, :, blocks], drecv.at[j, :, blocks], sent.at[3], d_r.at[j, i], partner
        )

    def first_hop(j, i, n):
        q, dev = (xq, xdev) if j % 2 == 0 else (yq, ydev)
        q = (q, dq)[n]
        blocks = pl.ds(i * nb, nb)
        return rdma(
            part.at[c, j, q, blocks], r1.at[j, n, blocks], sent.at[4], r1_r.at[j, i, n], dev
        )

    def second_hop(j, i):
        far, dev = (yq, ydev) if j % 2 == 0 else (xq, xdev)
        blocks = pl.ds(i * nb, nb)
        return rdma(
            part.at[c, j, far, blocks], r2.at[j, blocks], sent.at[5], r2_r.at[j], dev
        )

    def raw_copy(zz, j, i):
        blocks = pl.ds(i * nb, nb)
        m = moved.index(j)
        return rdma(
            part.at[c, j, :, blocks], raw.at[m, :, blocks], sent.at[10], raw_r.at[m, i],
            updev if zz == 0 else dndev,
        )

    def add_to(dst, src, start, count):
        step = next(n for n in (10, 8, 5, 4, 2, 1) if count % n == 0)

        def body(i, carry):
            sl = pl.ds(start + i * step, step)
            dst[sl] = (dst[sl].astype(F32) + src[sl].astype(F32)).astype(BF16)
            return carry

        lax.fori_loop(0, count // step, body, 0)

    def second_got(j):
        ref = r2.at[j]
        return rdma(ref, ref, sent.at[5], r2_r.at[j], partner)

    def z_copy(j, q, up, here):
        if up:
            return rdma(slots.at[j, q], zup.at[j, q], sent.at[6], z_r.at[j, q], updev)
        k = planes if q == here else q
        return rdma(slots.at[j, q], zdn.at[j, q], sent.at[7], z_r.at[j, k], dndev)

    my_id = quad * 2 + c

    def f_copies(zz, j):
        out = []
        for n, dev in enumerate(near):
            cc = oc if n in (0, 2, 4) else c
            onward_there = n in ((1, 2) if j % 2 == 0 else (3, 4))
            out.append(
                rdma(
                    slots.at[j, zz, pl.ds(cc * cap, cap)], frecv.at[j, my_id],
                    sent.at[8], pass_r.at[j] if onward_there else end_r, dev,
                )
            )
        return out

    def f_pass(j):
        q, dev = (xq, ydev) if j % 2 == 0 else (yq, xdev)
        pair = frecv.at[j, pl.ds(q * 2, 2)]
        return rdma(pair, pair, sent.at[8], end_r, dev)

    def f_pair(j):
        pair = frecv.at[j, pl.ds(0, 2)]
        return rdma(pair, pair, sent.at[8], pass_r.at[j], partner)

    def f_all(ss, rs, count):
        ref = frecv.at[:, pl.ds(0, count)]
        return rdma(ref, ref, ss, rs, partner)

    def g_copy(n):
        dev = (partner, xdev, ydev, ddev)[n]
        return rdma(gst.at[min(n, 1)], grecv.at[n], sent.at[9], g_r.at[n], dev)

    def gz_copy(d, q):
        return rdma(gst.at[2], gz.at[q], sent.at[9], gz_r, others[d - 1])

    def g_all(ref, ss, rs):
        return rdma(ref, ref, ss, rs, partner)

    def squares(i, acc):
        v = tok[:, pl.ds(pl.multiple_of(i * 2 * BLK, 2 * BLK), 2 * BLK)].astype(F32)
        v = v * v
        return acc + v[:, :BLK] + v[:, BLK:]

    def term(i, carry):
        cols = pl.ds(pl.multiple_of(i * wide, wide), wide)
        normed = (tok[:, cols].astype(F32) * inv[...] * gain[:, cols]).astype(BF16)
        res = lax.dot_general(
            normed, cot[...], (((0,), (0,)), ((), ())), preferred_element_type=F32
        )
        res = (res * scale).astype(BF16)
        group = res.shape[1] // (2 * QUAD)
        for b in range(wide // BLK):
            tgrad[i * (wide // BLK) + b] = normed[:, b * BLK:(b + 1) * BLK]
            for j in range(NJ):
                lo = b * BLK + j * SUB
                for k in range(QUAD):
                    for cc in range(2):
                        col = (k * 2 + cc) * group
                        part[cc, j, k, i * (wide // BLK) + b] = res[lo:lo + SUB, col:col + group]
        return carry

    def weight_group(g, grp):
        return jnp.concatenate([whole[slot_of[g * grp + i]] for i in range(grp)], axis=0)

    def cuts(grp, a):
        groups = nblk // grp
        return groups * a // COMPUTE, groups * (a + 1) // COMPUTE

    def fwd_body(q, core):
        first = (2 * q + core) * cap
        cols = []
        for u in range(cap):
            b = bos[first + u]
            val = tgrad[jnp.maximum(b, 0)]
            cols.append(jnp.where(b >= 0, val.astype(F32), 0.0).astype(BF16))
        rows = whole[pl.ds(first, cap)].reshape(cap * BLK, whole.shape[2])
        fwd[...] += jnp.dot(
            jnp.concatenate(cols, axis=1), rows, preferred_element_type=F32
        )

    def bwd_body(g, carry):
        gw = BGRP * BLK
        cols = pl.ds(pl.multiple_of(g * gw, gw), gw)
        grad = lax.dot_general(
            cot[...], weight_group(g, BGRP), (((1,), (1,)), ((), ())), preferred_element_type=F32
        )
        values = tok[:, cols].astype(F32)
        grad = grad * inv[...]
        out = (grad * gain[:, cols] - values * coef[...]).astype(BF16)
        for b in range(BGRP):
            tgrad[g * BGRP + b] = out[:, b * BLK:(b + 1) * BLK]
        gst[0, :, cols] = jnp.sum(grad * values, axis=0, keepdims=True) * scale
        return carry

    def shared_step(step, a):
        if step == SQ:
            loads[1].wait()
            acc = lax.fori_loop(
                0, width // (2 * BLK), squares, jnp.zeros((tokens_here, BLK), F32)
            )
            inv[...] = lax.rsqrt(jnp.sum(acc, axis=1, keepdims=True) / width + EPS)
            for cp in loads[2:5]:
                cp.wait()
        elif step == TERM:
            count = width // wide
            lax.fori_loop(a * count // NI, (a + 1) * count // NI, term, 0)
            for j in range(NJ):
                d_copy(j, a).start()
        elif step == FWD:
            if a == 0:
                fwd[...] = jnp.zeros_like(fwd)
            q = sum(jnp.where(z == zz, plans[zz][2][a], 0) for zz in range(planes))
            chunks_of(2 * cap, sent.at[2], agp_r.at[q]).wait_recv()

            def body(core, carry):
                fwd_body(q, core)
                return carry

            lax.fori_loop(0, 2, body, 0)
        else:
            if a == 0:
                total = fwd[...]
                proj[...] = (total + bias[...]).astype(BF16)
                inner = jnp.sum(total * cot[...].astype(F32), axis=1, keepdims=True) / width
                coef[...] = inv[...] * inv[...] * inner
                gst[0, :, width:] = jnp.sum(cot[...].astype(F32), axis=0, keepdims=True) * scale
            lax.fori_loop(*cuts(BGRP, a), bwd_body, 0)

    ends = (0, planes - 1)
    beside = (1, planes - 2)

    def own_step(zz, step, a, b):
        if step == OWN:
            for d in onward(zz, zz):
                ag_z(zz, d, a).start()
        elif step == OWNP:
            own_part().start()
        elif step == OWNER:
            lax.fori_loop(0, 2 * planes * cap, owner, 0)
        elif step == OWNX:
            ag_direct(zz, a, b).start()
        elif step == RAW:
            raw_copy(zz, a, b).start()
        elif step == AGZ:
            ag_z(a, 0, b).wait_recv()
            for d in onward(zz, a):
                ag_z(a, d, b).start()
            ag_part(a, 0, b).start()
        elif step == AGSIDE:
            ag_side(a, 0, b).start()
        elif step == AGPART:
            ag_side(a, 1, b).wait_recv()
            ag_part(a, 1, b).start()
        elif step == SUM:
            d_copy(a, b).wait_recv()
            for k in range(QUAD):
                add_to(part.at[c, a, k], drecv.at[a, k], b * nb, nb)
            if a in moved and zz in beside:
                raw_copy(zz, a, b).wait_recv()
                for k in range(QUAD):
                    add_to(part.at[c, a, k], raw.at[moved.index(a), k], b * nb, nb)
        elif step == HOP1:
            first_hop(a, b, 1).start()
            first_hop(a, b, 0).start()
        elif step == HOP2:
            far = yq if a % 2 == 0 else xq
            first_hop(a, b, 1).wait_recv()
            add_to(part.at[c, a, far], r1.at[a, 1], b * nb, nb)
            second_hop(a, b).start()
            first_hop(a, b, 0).wait_recv()
            add_to(part.at[c, a, quad], r1.at[a, 0], b * nb, nb)
        elif step == PLACE:
            second_got(a).wait_recv()
            add_to(part.at[c, a, quad], r2.at[a], 0, nblk)

            def body(i, carry):
                for u in range(per_plane):
                    k = bos[i * per_plane + u]
                    val = part[c, a, quad, jnp.maximum(k, 0)]
                    slots[a, i, u] = jnp.where(k >= 0, val.astype(F32), 0.0).astype(BF16)
                return carry

            lax.fori_loop(0, planes, body, 0)
        elif step == ZUP:
            if zz > (1 if a in moved else 0):
                z_copy(a, b, True, zz).wait_recv()
                add_to(slots.at[a, b], zup.at[a, b], 0, per_plane)
            z_copy(a, b, True, zz).start()
        elif step == ZDN:
            if zz < planes - (2 if a in moved else 1):
                z_copy(a, b, False, zz).wait_recv()
                add_to(slots.at[a, b], zdn.at[a, b], 0, per_plane)
            z_copy(a, b, False, zz - 1).start()
        elif step == ZEND:
            for up, buf in ((True, zup), (False, zdn)):
                hops = zz if up else planes - 1 - zz
                if hops > (1 if a in moved else 0) or (a in moved and hops == planes - 1):
                    z_copy(a, zz, up, zz).wait_recv()
                    if a in moved and zz in ends:
                        slots[a, zz] = buf[a, zz]
                    else:
                        add_to(slots.at[a, zz], buf.at[a, zz], 0, per_plane)
            for cp in f_copies(zz, a):
                cp.start()
            frecv[a, my_id] = slots[a, zz, pl.ds(c * cap, cap)]
        elif step == PASS:
            f_pair(a).wait_recv()
            f_pass(a).start()
        elif step == G0:
            g_copy(0).start()
        elif step == GSTEP:
            if a == 0:
                g_copy(0).wait_recv()
                gst[1] = gst[0] + grecv[0]
                for n in (3, 1, 2):
                    g_copy(n).start()
            else:
                for n in (1, 2, 3):
                    g_copy(n).wait_recv()
                gst[2] = (gst[1] + grecv[1]) + (grecv[2] + grecv[3])
                gz[zz] = gst[2]
                for d in range(1, planes):
                    gz_copy(d, zz).start()
        elif step == GEND:
            g_all(gz.at[pl.ds(0, planes - 1)], sent.at[9], gz_r).wait_recv()
            total = gz[0]
            for q in range(1, planes):
                total = total + gz[q]
            vec[...] = total

    def finish(zz):
        f_all(sent.at[8], end_r, 5).wait_recv()
        count = sum(len(onward(zz, q)) for q in range(planes)) * half
        count += len(direct(zz + 1, zz)) + len(direct(zz - 1, zz))
        chunks_of(count, sent.at[0], end_r).wait_send()
        count = (planes - 1) * half - len(direct(zz, zz - 1)) - len(direct(zz, zz + 1))
        chunks_of(count, sent.at[1], end_r).wait_send()
        chunks_of(2 * planes * cap, sent.at[2], end_r).wait_send()
        rdma(drecv, drecv, sent.at[3], end_r, partner).wait_send()
        pieces = NJ - (len(moved) if zz in ends else 0)
        for n, buf in ((4, r1), (5, r2)):
            ref = buf.at[pl.ds(0, pieces)]
            rdma(ref, ref, sent.at[n], end_r, partner).wait_send()
        if pieces < NJ:
            rdma(raw, raw, sent.at[10], end_r, partner).wait_send()
        for n, count in ((6, planes - 1 - zz), (7, zz)):
            if count:
                ref = slots.at[pl.ds(0, pieces), pl.ds(0, count)]
                rdma(ref, ref, sent.at[n], end_r, partner).wait_send()
        f_all(sent.at[8], end_r, 7).wait_send()
        g_all(gz.at[pl.ds(0, planes - 1)], sent.at[9], gz_r).wait_send()
        g_all(grecv, sent.at[9], gz_r).wait_send()

    plans = [split(order_of(zz, planes, cap)) for zz in range(planes)]
    common = plans[0][1]
    for n in range(len(common) + 1):
        for zz in range(planes):
            assert plans[zz][1] == common
            todo = plans[zz][0][n]
            last = n == len(common)
            if todo or last:
                @pl.when(z == zz)
                def _():
                    for tk in todo:
                        own_step(zz, *tk)
                    if last:
                        finish(zz)

        if n < len(common):
            shared_step(*common[n][:2])


def write_kernel(proj, tgrad, frecv, vec, proj_h, tgrad_h, wgrad_h, gain_h, bias_h, buf, sem):
    width = gain_h.shape[1]
    cap = frecv.shape[2]
    for b in range(tgrad.shape[0]):
        pltpu.make_async_copy(tgrad.at[b], tgrad_h.at[:, pl.ds(b * BLK, BLK)], sem.at[3]).start()
    copies = [
        pltpu.make_async_copy(proj, proj_h, sem.at[0]),
        pltpu.make_async_copy(vec.at[:, :width], gain_h, sem.at[1]),
        pltpu.make_async_copy(vec.at[:, width:], bias_h, sem.at[2]),
    ]
    for cp in copies:
        cp.start()
    for u in range(cap):
        for j in range(NJ):
            for n in range(2 * QUAD):
                buf[u, j * SUB:(j + 1) * SUB, n * BLK:(n + 1) * BLK] = frecv[j, n, u].astype(F32)
        pltpu.make_async_copy(buf.at[u], wgrad_h.at[u], sem.at[4]).start()
    for cp in copies:
        cp.wait()
    pltpu.make_async_copy(tgrad_h, tgrad_h, sem.at[3]).wait()
    pltpu.make_async_copy(buf, wgrad_h, sem.at[4]).wait()


def communicate(tokens, norm_gain, cotangent, key_bias, block_slot, key_weight, scale):
    shard_count = lax.axis_size("shard")
    planes = shard_count // 2
    rows, cols = key_weight.shape
    cap = rows // BLK
    raws = max(1, len(moved_of(planes, cap)))
    tok_count, width = tokens.shape
    nblk = width // BLK
    group = cols // (2 * QUAD)
    dma = pltpu.SemaphoreType.DMA
    vm = pltpu.VMEM
    hbm = pl.BlockSpec(memory_space=pl.ANY)
    local = pl.BlockSpec(memory_space=vm)
    held = pl.pallas_call(
        functools.partial(comm_kernel, planes, cap, nblk, scale),
        out_shape=(
            vm((tok_count, cols), BF16),
            vm((nblk, tok_count, BLK), BF16),
            vm((NJ, 2 * QUAD, cap, SUB, group), BF16),
            vm((1, width + cols), F32),
        ),
        in_specs=[hbm] * 5 + [pl.BlockSpec(memory_space=pltpu.SMEM)],
        out_specs=(local,) * 4,
        scratch_shapes=[
            vm((shard_count * cap, BLK, cols), BF16),
            vm((tok_count, width), BF16),
            vm((tok_count, cols), BF16),
            vm((1, width), F32),
            vm((1, cols), F32),
            vm((tok_count, 1), F32),
            vm((tok_count, 1), F32),
            vm((tok_count, cols), F32),
            vm((3, 1, width + cols), F32),
            vm((4, 1, width + cols), F32),
            vm((planes, 1, width + cols), F32),
            vm((2, NJ, QUAD, nblk, SUB, group), BF16),
            vm((NJ, QUAD, nblk, SUB, group), BF16),
            vm((NJ, 2, nblk, SUB, group), BF16),
            vm((NJ, nblk, SUB, group), BF16),
            vm((raws, QUAD, nblk, SUB, group), BF16),
            vm((NJ, planes, 2 * cap, SUB, group), BF16),
            vm((NJ, planes, 2 * cap, SUB, group), BF16),
            vm((NJ, planes, 2 * cap, SUB, group), BF16),
            pltpu.SMEM((shard_count * cap,), jnp.int32),
            dma((5,)),
            dma((planes, cap)), dma((planes, cap)), dma((planes,)),
            dma((NJ, NI)), dma((NJ, NI, 2)), dma((NJ,)), dma((raws, NI)), dma((NJ, planes + 1)),
            dma((NJ,)), dma(()), dma((4,)), dma(()), dma((11,)),
        ],
        compiler_params=pltpu.CompilerParams(
            collective_id=0, has_side_effects=True, vmem_limit_bytes=54 * 2**20
        ),
    )(
        tokens, norm_gain[None, :], cotangent, key_bias[None, :],
        key_weight.reshape(cap, BLK, cols), block_slot,
    )
    return pl.pallas_call(
        write_kernel,
        out_shape=(
            jax.ShapeDtypeStruct((tok_count, cols), BF16),
            jax.ShapeDtypeStruct((tok_count, width), BF16),
            jax.ShapeDtypeStruct((cap, BLK, cols), F32),
            jax.ShapeDtypeStruct((1, width), F32),
            jax.ShapeDtypeStruct((1, cols), F32),
        ),
        in_specs=[local] * 4,
        out_specs=(hbm,) * 5,
        scratch_shapes=[vm((cap, BLK, cols), F32), dma((5,))],
        compiler_params=pltpu.CompilerParams(vmem_limit_bytes=8 * 2**20),
    )(*held)


def local(tokens, norm_gain, key_bias, key_weight, cotangent, block_slot):
    row_count, width = tokens.shape
    shard_count = lax.axis_size("shard")
    replicas = lax.axis_size("rep")
    grad_scale = float(row_count * shard_count * replicas) ** (-0.5)
    projected, token_grad, weight_grad, gain_grad, bias_grad = communicate(
        tokens, norm_gain, cotangent, key_bias, block_slot, key_weight, grad_scale
    )
    weight_grad = weight_grad.reshape(key_weight.shape)
    if replicas > QUAD:
        groups = [list(range(i, replicas, QUAD)) for i in range(QUAD)]
        weight_grad, gain_grad, bias_grad = lax.psum(
            (weight_grad, gain_grad, bias_grad), "rep", axis_index_groups=groups
        )
    return (projected, token_grad, weight_grad, gain_grad[0], bias_grad[0])


def solution(mesh):
    return jax.shard_map(
        local,
        mesh=mesh,
        in_specs=(
            P(("shard", "rep"), None),
            P(),
            P(),
            P("shard", None),
            P(("shard", "rep"), None),
            P(),
        ),
        out_specs=(
            P(("shard", "rep"), None),
            P(("shard", "rep"), None),
            P("shard", None),
            P(),
            P(),
        ),
        check_vma=False,
    )
```
